128 devices in a mesh: lat: 4 (over x_hi, core), lon: 4 (over z), lev: 8 (over y, x_lo).
Axes of the slice: x: 4 (x_hi: 2, x_lo: 2; x = x_hi * 2 + x_lo), y: 4, z: 4, core: 2. Of those that a mesh axis runs over, the one named last changes fastest.
Arguments:
- initial_heat: float32 [128, 512, 32, 128], P('lat', 'lon', 'lev'), may hold values from 0.5 to 2
- diffusivity_ratio: float32 [128, 512, 32, 128], P('lat', 'lon', 'lev'), may hold values from 0.03 to 0.15
- forcing_term: float32 [128, 512, 32, 128], P('lat', 'lon', 'lev'), may hold values from -0.2 to 0.2
Outputs:
- standard_deviation_score: float32 [128, 512, 32, 128], P('lat', 'lon', 'lev')
- temperature_end: float32 [128, 512, 32, 128], P('lat', 'lon', 'lev')
The draws below stay inside these ranges and needn't reach their ends.
All inputs are finite; a program needn't handle non-finite values.
Results may differ from the reference program's by a relative error of at most 0.00002.
Values sent between devices are 32-bit elements; how exact they have to be, the bound alone decides.
A program may use at most 128 MiB of HBM per device.

```python
import jax
import jax.numpy as jnp
from jax import lax

GRID_DEPTH = 128
GRID_WIDTH = 512
GRID_HEIGHT = 32
MEMBER_TOTAL = 128
STEPS = 4


def steps_of(key, shape, cuts, least, top_value):
    level = 1.0
    for dim, shards_of in cuts:
        draws = jax.random.uniform(jax.random.fold_in(jax.random.fold_in(key, 6), dim), (shards_of,), jnp.float32, least / len(cuts), top_value / len(cuts))
        level = level * jnp.repeat(jnp.exp(draws), shape[dim] // shards_of).reshape((-1,) + (1,) * (len(shape) - 1 - dim))
    return level


def setup_inputs(seed: int = 0) -> dict:
    key_of = jax.random.split(jax.random.key(seed), 4)
    return {
        "initial_heat": jnp.clip(0.5 + 1.5 * jax.random.uniform(key_of[0], (GRID_DEPTH, GRID_WIDTH, GRID_HEIGHT, MEMBER_TOTAL), jnp.float32) ** steps_of(key_of[0], (GRID_DEPTH, GRID_WIDTH, GRID_HEIGHT, MEMBER_TOTAL), ((0, 4), (1, 4), (2, 8)), -0.2, 0.2), 0.5, 2.0),
        "diffusivity_ratio": jnp.clip(0.03 + 0.120000007 * jax.random.uniform(key_of[1], (GRID_DEPTH, GRID_WIDTH, GRID_HEIGHT, MEMBER_TOTAL), jnp.float32) ** steps_of(key_of[1], (GRID_DEPTH, GRID_WIDTH, GRID_HEIGHT, MEMBER_TOTAL), ((0, 4), (1, 4), (2, 8)), -0.2, 0.2), 0.03, 0.15),
        "forcing_term": jnp.clip(jax.random.uniform(key_of[2], (GRID_DEPTH, GRID_WIDTH, GRID_HEIGHT, MEMBER_TOTAL), jnp.float32, -0.2, 0.2) * steps_of(key_of[2], (GRID_DEPTH, GRID_WIDTH, GRID_HEIGHT, MEMBER_TOTAL), ((0, 4), (1, 4), (2, 8)), -0.4, 0.0), -0.2, 0.2),
    }


def without_rim(values, dims):
    for dim in dims:
        values = lax.slice_in_dim(values, 1, values.shape[dim] - 1, axis=dim)
    return values

def shifted_cells(values, dim, start, dims):
    others = [other for other in dims if other != dim]
    values = without_rim(values, others)
    return lax.slice_in_dim(values, start, start + values.shape[dim] - 2, axis=dim)

def march_forward(extended_grid_state, diffusivity_ratio, forcing_term):
    middle = without_rim(extended_grid_state, (0, 1, 2))
    lower = [shifted_cells(extended_grid_state, dim, 0, (0, 1, 2)) for dim in (0, 1, 2)]
    upper = [shifted_cells(extended_grid_state, dim, 2, (0, 1, 2)) for dim in (0, 1, 2)]
    spread = lower[0] + upper[0] + lower[1] + upper[1] + lower[2] + upper[2] - 6.0 * middle
    return middle + diffusivity_ratio * spread + forcing_term

def reference(initial_heat, diffusivity_ratio, forcing_term):
    for step in range(STEPS):
        initial_heat = march_forward(jnp.pad(initial_heat, ((1, 1), (1, 1), (1, 1), (0, 0)), mode='wrap'), diffusivity_ratio, forcing_term)
    row_mean_estimate = lax.optimization_barrier(jnp.mean(initial_heat, axis=1, keepdims=True))
    deviations_from_mean = initial_heat - row_mean_estimate
    line_variance = lax.optimization_barrier(jnp.mean(deviations_from_mean * deviations_from_mean, axis=1, keepdims=True))
    standard_deviation_score = deviations_from_mean * lax.rsqrt(line_variance + 0.0001)
    return (standard_deviation_score, initial_heat)
```

```python
import functools

import jax
import jax.numpy as jnp
from jax import lax
from jax.experimental import pallas as pl
from jax.experimental.pallas import tpu as pltpu
from jax.sharding import PartitionSpec as P

STEPS = 4
CHUNKS = 8
MESH = pl.DeviceIdType.MESH


def kernel(
    sizes,
    heat_hbm,
    ratio_hbm,
    force_hbm,
    score,
    final,
    u,
    ratio,
    force,
    lon_out,
    lon_in,
    stat_out,
    stat_in,
    load_sem,
    lev_send,
    lev_recv,
    lon_send,
    lon_recv,
    lat_send,
    lat_recv,
    stat_send,
    stat_recv,
):
    lat_size, lon_size, lev_size = sizes
    rows, wide, height = u.shape[2] - 2, u.shape[3], u.shape[1] - 2
    per = rows // CHUNKS
    lat, lon, lev = (lax.axis_index(a) for a in ("lat", "lon", "lev"))
    after = {
        "lat": lax.rem(lat + 1, lat_size),
        "lon": lax.rem(lon + 1, lon_size),
        "lev": lax.rem(lev + 1, lev_size),
    }
    before = {
        "lat": lax.rem(lat + lat_size - 1, lat_size),
        "lon": lax.rem(lon + lon_size - 1, lon_size),
        "lev": lax.rem(lev + lev_size - 1, lev_size),
    }
    first_cell = lax.broadcasted_iota(jnp.int32, (wide, 128), 0) == 0
    last_cell = lax.broadcasted_iota(jnp.int32, (wide, 128), 0) == wide - 1

    def chunk_rows(c, offset=0):
        return pl.ds(c * per + offset, per)

    def load(i, c):
        src = (heat_hbm, ratio_hbm, force_hbm)[i]
        dst = (score, ratio, force)[i]
        return pltpu.make_async_copy(
            src.at[chunk_rows(c)], dst.at[chunk_rows(c)], load_sem.at[i, c]
        )

    def target(axis, d):
        return {axis: (before, after)[d][axis]}

    def lev_copy(p, d, c):
        src, dst = ((1, height + 1), (height, 0))[d]
        return pltpu.make_async_remote_copy(
            src_ref=u.at[p, src, chunk_rows(c, 1)],
            dst_ref=u.at[p, dst, chunk_rows(c, 1)],
            send_sem=lev_send.at[p, d, c],
            recv_sem=lev_recv.at[p, d, c],
            device_id=target("lev", d),
            device_id_type=MESH,
        )

    def lat_copy(p, d):
        src, dst = ((1, rows + 1), (rows, 0))[d]
        return pltpu.make_async_remote_copy(
            src_ref=u.at[p, pl.ds(1, height), src],
            dst_ref=u.at[p, pl.ds(1, height), dst],
            send_sem=lat_send.at[p, d],
            recv_sem=lat_recv.at[p, d],
            device_id=target("lat", d),
            device_id_type=MESH,
        )

    def lon_copy(p, d, c):
        return pltpu.make_async_remote_copy(
            src_ref=lon_out.at[p, d, chunk_rows(c)],
            dst_ref=lon_in.at[p, d, chunk_rows(c)],
            send_sem=lon_send.at[p, d, c],
            recv_sem=lon_recv.at[p, d, c],
            device_id=target("lon", d),
            device_id_type=MESH,
        )

    def stat_copy(j, c):
        return pltpu.make_async_remote_copy(
            src_ref=stat_out.at[chunk_rows(c)],
            dst_ref=stat_in.at[j, chunk_rows(c)],
            send_sem=stat_send.at[j, c],
            recv_sem=stat_recv.at[j, c],
            device_id={"lon": lax.rem(lon + j + 1, lon_size)},
            device_id_type=MESH,
        )

    def order(k):
        return lax.rem(k + CHUNKS - 1, CHUNKS)

    def on_edges(c, low, high):
        pl.when(c == 0)(low)
        pl.when(c == CHUNKS - 1)(high)

    def send_faces(p, c):
        on_edges(c, lambda: lat_copy(p, 0).start(), lambda: lat_copy(p, 1).start())
        for d in (0, 1):
            lev_copy(p, d, c).start()
        for d in (0, 1):
            lon_copy(p, d, c).start()

    def wait_sent(p, c):
        on_edges(c, lambda: lat_copy(p, 0).wait_send(), lambda: lat_copy(p, 1).wait_send())
        for d in (0, 1):
            lev_copy(p, d, c).wait_send()
            lon_copy(p, d, c).wait_send()

    def wait_faces(p, c):
        on_edges(c, lambda: lat_copy(p, 1).wait_recv(), lambda: lat_copy(p, 0).wait_recv())
        for d in (0, 1):
            lev_copy(p, d, c).wait_recv()
            lon_copy(p, d, c).wait_recv()

    def put(p, y, z, values):
        u[p, z + 1, y + 1] = values
        lon_out[p, 0, y, z] = values[0]
        lon_out[p, 1, y, z] = values[wide - 1]

    def cells(z):
        return pl.ds(z, wide, stride=height)

    def stepped(p, y, z):
        middle = u[p, z + 1, y + 1]
        west = jnp.where(first_cell, lon_in[p, 1, y, pl.ds(z, 1)], pltpu.roll(middle, 1, 0))
        east = jnp.where(last_cell, lon_in[p, 0, y, pl.ds(z, 1)], pltpu.roll(middle, wide - 1, 0))
        spread = (
            (u[p, z + 1, y] + u[p, z + 1, y + 2])
            + (west + east)
            + (u[p, z, y + 1] + u[p, z + 2, y + 1])
            - 6.0 * middle
        )
        return middle + ratio[y, cells(z)] * spread + force[y, cells(z)]

    def each_row(c, body):
        def one(i, carry):
            body(c * per + i)
            return carry

        lax.fori_loop(0, per, one, 0)

    def each_chunk(body):
        def one(k, carry):
            body(k, order(k))
            return carry

        lax.fori_loop(0, CHUNKS, one, 0)

    each_chunk(lambda k, c: load(0, c).start())
    for i in (1, 2):
        each_chunk(lambda k, c, i=i: load(i, c).start())

    barrier = pltpu.get_barrier_semaphore()
    greeted = [{a: n[a]} for a in ("lat", "lev") for n in (before, after)]
    greeted += [{"lon": lax.rem(lon + j + 1, lon_size)} for j in range(lon_size - 1)]
    for other in greeted:
        pl.semaphore_signal(barrier, inc=1, device_id=other, device_id_type=MESH)
    pl.semaphore_wait(barrier, len(greeted))

    def begin(k, c):
        load(0, c).wait()

        def one(y):
            for z in range(height):
                put(0, y, z, score[y, cells(z)])

        each_row(c, one)
        send_faces(0, c)

    each_chunk(begin)

    for step in range(1, STEPS):
        p, q = (step - 1) % 2, step % 2

        def advance(k, c, step=step, p=p, q=q):
            if step == 1:
                load(1, c).wait()
                load(2, c).wait()
            else:
                wait_sent(q, c)
            wait_faces(p, c)

            def one(y):
                for z in range(height):
                    put(q, y, z, stepped(p, y, z))

            each_row(c, one)
            send_faces(q, c)

        each_chunk(advance)

    p, q = (STEPS - 1) % 2, STEPS % 2

    def finish(c):
        for j in range(lon_size - 1):
            stat_copy(j, c).wait_recv()

        def one(y):
            own = stat_out[y]
            others = [stat_in[j, y] for j in range(lon_size - 1)]
            summed = own
            for other in others:
                summed = summed + other
            mean = summed[:height] / lon_size
            apart = (own[:height] - mean) * (own[:height] - mean)
            for other in others:
                apart = apart + (other[:height] - mean) * (other[:height] - mean)
            variance = summed[height:] / (lon_size * wide) + apart / lon_size
            scale = lax.rsqrt(variance + 0.0001)
            for z in range(height):
                score[y, cells(z)] = (u[q, z + 1, y + 1] - mean[z : z + 1]) * scale[z : z + 1]

        each_row(c, one)

    def last(k, c):
        wait_sent(q, c)
        wait_faces(p, c)

        def one(y):
            for z in range(height):
                values = stepped(p, y, z)
                u[q, z + 1, y + 1] = values
                final[y, cells(z)] = values
                mean = jnp.sum(values, axis=0, keepdims=True) / wide
                apart = values - mean
                stat_out[y, pl.ds(z, 1)] = mean
                stat_out[y, pl.ds(height + z, 1)] = jnp.sum(apart * apart, axis=0, keepdims=True)

        each_row(c, one)
        for j in range(lon_size - 1):
            stat_copy(j, c).start()
        pl.when(k > 0)(lambda: finish(order(k + CHUNKS - 1)))

    each_chunk(last)
    finish(order(CHUNKS - 1))

    def settle(k, c):
        wait_sent(p, c)
        for j in range(lon_size - 1):
            stat_copy(j, c).wait_send()

    each_chunk(settle)


def local(sizes, initial_heat, diffusivity_ratio, forcing_term):
    rows, wide, height, members = initial_heat.shape
    flat = (rows, wide * height, members)
    hbm = pl.BlockSpec(memory_space=pl.ANY)
    vmem = pl.BlockSpec(memory_space=pltpu.VMEM)
    f32, dma = jnp.float32, pltpu.SemaphoreType.DMA
    lon_size = sizes[1]
    score, final = pl.pallas_call(
        functools.partial(kernel, sizes),
        out_shape=(jax.ShapeDtypeStruct(flat, f32), jax.ShapeDtypeStruct(flat, f32)),
        in_specs=[hbm, hbm, hbm],
        out_specs=(vmem, vmem),
        scratch_shapes=[
            pltpu.VMEM((2, height + 2, rows + 2, wide, members), f32),
            pltpu.VMEM(flat, f32),
            pltpu.VMEM(flat, f32),
            pltpu.VMEM((2, 2, rows, height, members), f32),
            pltpu.VMEM((2, 2, rows, height, members), f32),
            pltpu.VMEM((rows, 2 * height, members), f32),
            pltpu.VMEM((lon_size - 1, rows, 2 * height, members), f32),
            dma((3, CHUNKS)),
            dma((2, 2, CHUNKS)),
            dma((2, 2, CHUNKS)),
            dma((2, 2, CHUNKS)),
            dma((2, 2, CHUNKS)),
            dma((2, 2)),
            dma((2, 2)),
            dma((lon_size - 1, CHUNKS)),
            dma((lon_size - 1, CHUNKS)),
        ],
        compiler_params=pltpu.CompilerParams(
            collective_id=0, has_side_effects=True, vmem_limit_bytes=63 * 2**20
        ),
    )(*(a.reshape(flat) for a in (initial_heat, diffusivity_ratio, forcing_term)))
    return score.reshape(initial_heat.shape), final.reshape(initial_heat.shape)


def solution(mesh):
    sizes = tuple(mesh.shape[a] for a in ("lat", "lon", "lev"))
    placed = P("lat", "lon", "lev", None)
    return jax.shard_map(
        functools.partial(local, sizes),
        mesh=mesh,
        in_specs=(placed, placed, placed),
        out_specs=(placed, placed),
        check_vma=False,
    )
```

```python
import functools

import jax
import jax.numpy as jnp
from jax import lax
from jax.experimental import pallas as pl
from jax.experimental.pallas import tpu as pltpu
from jax.sharding import PartitionSpec as P

STEPS = 4
CHUNKS = 8
MESH = pl.DeviceIdType.MESH


def kernel(
    sizes,
    heat_hbm,
    ratio_hbm,
    force_hbm,
    score,
    final,
    u,
    ratio,
    force,
    lon_out,
    lon_in,
    stat_out,
    stat_in,
    load_sem,
    lev_send,
    lev_recv,
    lon_send,
    lon_recv,
    lat_send,
    lat_recv,
    stat_send,
    stat_recv,
):
    lat_size, lon_size, lev_size = sizes
    rows, wide, height = u.shape[2] - 2, u.shape[3], u.shape[1] - 2
    per = rows // CHUNKS
    lat, lon, lev = (lax.axis_index(a) for a in ("lat", "lon", "lev"))
    after = {
        "lat": lax.rem(lat + 1, lat_size),
        "lon": lax.rem(lon + 1, lon_size),
        "lev": lax.rem(lev + 1, lev_size),
    }
    before = {
        "lat": lax.rem(lat + lat_size - 1, lat_size),
        "lon": lax.rem(lon + lon_size - 1, lon_size),
        "lev": lax.rem(lev + lev_size - 1, lev_size),
    }
    first_cell = lax.broadcasted_iota(jnp.int32, (wide, 128), 0) == 0
    last_cell = lax.broadcasted_iota(jnp.int32, (wide, 128), 0) == wide - 1

    def chunk_rows(c, offset=0):
        return pl.ds(c * per + offset, per)

    def load(i, c):
        src = (heat_hbm, ratio_hbm, force_hbm)[i]
        dst = (score, ratio, force)[i]
        return pltpu.make_async_copy(
            src.at[chunk_rows(c)], dst.at[chunk_rows(c)], load_sem.at[i, c]
        )

    def target(axis, d):
        return {axis: (before, after)[d][axis]}

    def lev_copy(p, d, c):
        src, dst = ((1, height + 1), (height, 0))[d]
        return pltpu.make_async_remote_copy(
            src_ref=u.at[p, src, chunk_rows(c, 1)],
            dst_ref=u.at[p, dst, chunk_rows(c, 1)],
            send_sem=lev_send.at[p, d, c],
            recv_sem=lev_recv.at[p, d, c],
            device_id=target("lev", d),
            device_id_type=MESH,
        )

    def lat_copy(p, d):
        src, dst = ((1, rows + 1), (rows, 0))[d]
        return pltpu.make_async_remote_copy(
            src_ref=u.at[p, pl.ds(1, height), src],
            dst_ref=u.at[p, pl.ds(1, height), dst],
            send_sem=lat_send.at[p, d],
            recv_sem=lat_recv.at[p, d],
            device_id=target("lat", d),
            device_id_type=MESH,
        )

    def lon_copy(p, d, c):
        return pltpu.make_async_remote_copy(
            src_ref=lon_out.at[p, d, chunk_rows(c)],
            dst_ref=lon_in.at[p, d, chunk_rows(c)],
            send_sem=lon_send.at[p, d, c],
            recv_sem=lon_recv.at[p, d, c],
            device_id=target("lon", d),
            device_id_type=MESH,
        )

    def stat_copy(j, c):
        return pltpu.make_async_remote_copy(
            src_ref=stat_out.at[chunk_rows(c)],
            dst_ref=stat_in.at[j, chunk_rows(c)],
            send_sem=stat_send.at[j, c],
            recv_sem=stat_recv.at[j, c],
            device_id={"lon": lax.rem(lon + j + 1, lon_size)},
            device_id_type=MESH,
        )

    def order(k):
        return lax.rem(k + CHUNKS - 1, CHUNKS)

    def on_edges(c, low, high):
        pl.when(c == 0)(low)
        pl.when(c == CHUNKS - 1)(high)

    def send_faces(p, c):
        on_edges(c, lambda: lat_copy(p, 0).start(), lambda: lat_copy(p, 1).start())
        for d in (0, 1):
            lev_copy(p, d, c).start()
        for d in (0, 1):
            lon_copy(p, d, c).start()

    def wait_sent(p, c):
        on_edges(c, lambda: lat_copy(p, 0).wait_send(), lambda: lat_copy(p, 1).wait_send())
        for d in (0, 1):
            lev_copy(p, d, c).wait_send()
            lon_copy(p, d, c).wait_send()

    def wait_faces(p, c):
        on_edges(c, lambda: lat_copy(p, 1).wait_recv(), lambda: lat_copy(p, 0).wait_recv())
        for d in (0, 1):
            lev_copy(p, d, c).wait_recv()
            lon_copy(p, d, c).wait_recv()

    def put(p, y, z, values):
        u[p, z + 1, y + 1] = values
        lon_out[p, 0, y, z] = values[0]
        lon_out[p, 1, y, z] = values[wide - 1]

    def cells(z):
        return pl.ds(z, wide, stride=height)

    def stepped(p, y, z):
        middle = u[p, z + 1, y + 1]
        west = jnp.where(first_cell, lon_in[p, 1, y, pl.ds(z, 1)], pltpu.roll(middle, 1, 0))
        east = jnp.where(last_cell, lon_in[p, 0, y, pl.ds(z, 1)], pltpu.roll(middle, wide - 1, 0))
        spread = (
            (u[p, z + 1, y] + u[p, z + 1, y + 2])
            + (west + east)
            + (u[p, z, y + 1] + u[p, z + 2, y + 1])
            - 6.0 * middle
        )
        return middle + ratio[y, cells(z)] * spread + force[y, cells(z)]

    def each_row(c, body):
        def one(i, carry):
            body(c * per + i)
            return carry

        lax.fori_loop(0, per, one, 0)

    def each_chunk(body):
        def one(k, carry):
            body(k, order(k))
            return carry

        lax.fori_loop(0, CHUNKS, one, 0)

    each_chunk(lambda k, c: load(0, c).start())

    barrier = pltpu.get_barrier_semaphore()
    greeted = [{a: n[a]} for a in ("lat", "lev") for n in (before, after)]
    greeted += [{"lon": lax.rem(lon + j + 1, lon_size)} for j in range(lon_size - 1)]
    for other in greeted:
        pl.semaphore_signal(barrier, inc=1, device_id=other, device_id_type=MESH)

    def begin(k, c):
        load(0, c).wait()

        def one(y):
            for z in range(height):
                put(0, y, z, score[y, cells(z)])

        each_row(c, one)
        pl.when(k == 0)(lambda: pl.semaphore_wait(barrier, len(greeted)))
        send_faces(0, c)
        for i in (1, 2):
            load(i, c).start()

    each_chunk(begin)

    for step in range(1, STEPS):
        p, q = (step - 1) % 2, step % 2

        def advance(k, c, step=step, p=p, q=q):
            if step == 1:
                load(1, c).wait()
                load(2, c).wait()
            else:
                wait_sent(q, c)
            wait_faces(p, c)

            def one(y):
                for z in range(height):
                    put(q, y, z, stepped(p, y, z))

            each_row(c, one)
            send_faces(q, c)

        each_chunk(advance)

    p, q = (STEPS - 1) % 2, STEPS % 2

    def finish(c):
        for j in range(lon_size - 1):
            stat_copy(j, c).wait_recv()

        def one(y):
            own = stat_out[y]
            others = [stat_in[j, y] for j in range(lon_size - 1)]
            summed = own
            for other in others:
                summed = summed + other
            mean = summed[:height] / lon_size
            apart = (own[:height] - mean) * (own[:height] - mean)
            for other in others:
                apart = apart + (other[:height] - mean) * (other[:height] - mean)
            variance = summed[height:] / (lon_size * wide) + apart / lon_size
            scale = lax.rsqrt(variance + 0.0001)
            for z in range(height):
                score[y, cells(z)] = (u[q, z + 1, y + 1] - mean[z : z + 1]) * scale[z : z + 1]

        each_row(c, one)

    def last(k, c):
        wait_sent(q, c)
        wait_faces(p, c)

        def one(y):
            for z in range(height):
                values = stepped(p, y, z)
                u[q, z + 1, y + 1] = values
                final[y, cells(z)] = values
                mean = jnp.sum(values, axis=0, keepdims=True) / wide
                apart = values - mean
                stat_out[y, pl.ds(z, 1)] = mean
                stat_out[y, pl.ds(height + z, 1)] = jnp.sum(apart * apart, axis=0, keepdims=True)

        each_row(c, one)
        for j in range(lon_size - 1):
            stat_copy(j, c).start()
        pl.when(k > 0)(lambda: finish(order(k + CHUNKS - 1)))

    each_chunk(last)
    finish(order(CHUNKS - 1))

    def settle(k, c):
        wait_sent(p, c)
        for j in range(lon_size - 1):
            stat_copy(j, c).wait_send()

    each_chunk(settle)


def write_out(score, final, score_hbm, final_hbm, sem):
    copies = [
        pltpu.make_async_copy(score, score_hbm, sem.at[0]),
        pltpu.make_async_copy(final, final_hbm, sem.at[1]),
    ]
    for copy in copies:
        copy.start()
    for copy in copies:
        copy.wait()


def local(sizes, initial_heat, diffusivity_ratio, forcing_term):
    rows, wide, height, members = initial_heat.shape
    flat = (rows, wide * height, members)
    hbm = pl.BlockSpec(memory_space=pl.ANY)
    vmem = pl.BlockSpec(memory_space=pltpu.VMEM)
    f32, dma = jnp.float32, pltpu.SemaphoreType.DMA
    lon_size = sizes[1]
    score, final = pl.pallas_call(
        functools.partial(kernel, sizes),
        out_shape=(pltpu.VMEM(flat, f32), pltpu.VMEM(flat, f32)),
        in_specs=[hbm, hbm, hbm],
        out_specs=(vmem, vmem),
        scratch_shapes=[
            pltpu.VMEM((2, height + 2, rows + 2, wide, members), f32),
            pltpu.VMEM(flat, f32),
            pltpu.VMEM(flat, f32),
            pltpu.VMEM((2, 2, rows, height, members), f32),
            pltpu.VMEM((2, 2, rows, height, members), f32),
            pltpu.VMEM((rows, 2 * height, members), f32),
            pltpu.VMEM((lon_size - 1, rows, 2 * height, members), f32),
            dma((3, CHUNKS)),
            dma((2, 2, CHUNKS)),
            dma((2, 2, CHUNKS)),
            dma((2, 2, CHUNKS)),
            dma((2, 2, CHUNKS)),
            dma((2, 2)),
            dma((2, 2)),
            dma((lon_size - 1, CHUNKS)),
            dma((lon_size - 1, CHUNKS)),
        ],
        compiler_params=pltpu.CompilerParams(
            collective_id=0, has_side_effects=True, vmem_limit_bytes=46 * 2**20
        ),
    )(*(a.reshape(flat) for a in (initial_heat, diffusivity_ratio, forcing_term)))
    score, final = pl.pallas_call(
        write_out,
        out_shape=(jax.ShapeDtypeStruct(flat, f32), jax.ShapeDtypeStruct(flat, f32)),
        in_specs=[vmem, vmem],
        out_specs=(hbm, hbm),
        scratch_shapes=[dma((2,))],
        compiler_params=pltpu.CompilerParams(vmem_limit_bytes=4 * 2**20),
    )(*(pltpu.with_memory_space_constraint(a, pltpu.VMEM) for a in (score, final)))
    return score.reshape(initial_heat.shape), final.reshape(initial_heat.shape)


def solution(mesh):
    sizes = tuple(mesh.shape[a] for a in ("lat", "lon", "lev"))
    placed = P("lat", "lon", "lev", None)
    return jax.shard_map(
        functools.partial(local, sizes),
        mesh=mesh,
        in_specs=(placed, placed, placed),
        out_specs=(placed, placed),
        check_vma=False,
    )
```

```python
import functools

import jax
import jax.numpy as jnp
from jax import lax
from jax.experimental import pallas as pl
from jax.experimental.pallas import tpu as pltpu
from jax.sharding import PartitionSpec as P

STEPS = 4
DEPTH = 2
SLOTS = 2
PARTS = 8
MESH = pl.DeviceIdType.MESH


def kernel(
    sizes,
    heat_hbm,
    ratio_hbm,
    force_hbm,
    score,
    final,
    u,
    ratio,
    force,
    packed,
    lat_in,
    lat_held,
    lon_out,
    lon_in,
    stat_out,
    stat_in,
    moment_out,
    moment_in,
    load_sem,
    swap_send,
    swap_recv,
    back_send,
    back_recv,
    lev_send,
    lev_recv,
    lon_send,
    lon_recv,
    lat_send,
    lat_recv,
    stat_send,
    stat_recv,
    moment_send,
    moment_recv,
):
    lat_size, lon_size, lev_size = sizes
    rows = final.shape[0]
    chunks, slab, members = u.shape[2:]
    height = u.shape[1] - 2
    pairs = height // 2
    wide = slab // (2 * DEPTH)
    lines = 2 * DEPTH
    lat, lon, lev = (lax.axis_index(a) for a in ("lat", "lon", "lev"))
    kind = lax.rem(lev, 2)
    outer_x = lat // (lat_size // 2)
    half = lax.rem(kind + outer_x, 2)
    partner_lev = lev + 1 - 2 * kind

    lane = lax.broadcasted_iota(jnp.int32, (wide, members), 1)
    line = lax.broadcasted_iota(jnp.int32, (wide, members), 0)
    low_lanes = lane < members // 2
    first_cell = line == 0
    last_cell = line == wide - 1

    def lat_target(d):
        other = lax.rem(lat + (lat_size - 1, 1)[d], lat_size)
        crossed = lax.rem(other // (lat_size // 2) + outer_x, 2)
        return {"lat": other, "lev": lev + crossed * (1 - 2 * kind)}

    def lev_target(d):
        return {"lev": lax.rem(lev + (lev_size - 2, 2)[d], lev_size)}

    def lon_target(d):
        return {"lon": lax.rem(lon + (lon_size - 1, 1)[d], lon_size)}

    def stat_target(j):
        return {"lon": lax.rem(lon + j + 1, lon_size)}

    def swapped(x):
        return pltpu.roll(x, members // 2, 1)

    def butterfly(a, b):
        return jnp.where(low_lanes, a, swapped(b)), jnp.where(low_lanes, swapped(a), b)

    def remote(src, dst, send_sem, recv_sem, target):
        return pltpu.make_async_remote_copy(
            src_ref=src,
            dst_ref=dst,
            send_sem=send_sem,
            recv_sem=recv_sem,
            device_id=target,
            device_id_type=MESH,
        )

    def row_of(c, i, side):
        return c * DEPTH + i if side == 0 else rows - 1 - c * DEPTH - i

    def staged(c, f, side):
        return (lax.rem(c, 2) * 3 + f) * lines + side * DEPTH

    def load(f, c, side):
        src = (heat_hbm, ratio_hbm, force_hbm)[f]
        first = c * DEPTH if side == 0 else rows - (c + 1) * DEPTH
        return pltpu.make_async_copy(
            src.at[pl.ds(first, DEPTH)],
            final.at[pl.ds(staged(c, f, side), DEPTH)],
            load_sem.at[f, side, lax.rem(c, 2)],
        )

    def plane(f, z):
        return (u.at[0, 1 + z], ratio.at[z], force.at[z])[f]

    def swap_copy(f, i, c):
        slot = lax.rem(c, SLOTS)
        return remote(
            packed.at[slot, f, i],
            plane(f, 2 * i + kind).at[c],
            swap_send.at[slot, f, i],
            swap_recv.at[c, f, i],
            {"lev": partner_lev},
        )

    def back_copy(i, c):
        return remote(
            ratio.at[2 * i + 1 - kind, c],
            score.at[c * pairs + i],
            back_send.at[c, i],
            back_recv.at[c, i],
            {"lev": partner_lev},
        )

    def lev_copy(p, d, c):
        src, dst = ((1, height + 1), (height, 0))[d]
        return remote(
            u.at[p, src, c],
            u.at[p, dst, c],
            lev_send.at[p, d, c],
            lev_recv.at[p, d, c],
            lev_target(d),
        )

    def lat_copy(p, d):
        return remote(
            u.at[p, pl.ds(1, height), 0, pl.ds(d * wide, wide)],
            lat_in.at[p, 1 - d],
            lat_send.at[p, d],
            lat_recv.at[p, d],
            lat_target(d),
        )

    def lon_copy(p, d, c):
        return remote(
            lon_out.at[p, d, c],
            lon_in.at[p, d, c],
            lon_send.at[p, d, c],
            lon_recv.at[p, d, c],
            lon_target(d),
        )

    def stat_copy(j, c):
        return remote(
            stat_out.at[c],
            stat_in.at[j, c],
            stat_send.at[j, c],
            stat_recv.at[j, c],
            stat_target(j),
        )

    def at_edge(c, body):
        @pl.when(c == 0)
        def _():
            for d in (0, 1):
                body(d)

    def send_faces(p, c):
        at_edge(c, lambda d: lat_copy(p, d).start())
        for d in (0, 1):
            lev_copy(p, d, c).start()
        for d in (0, 1):
            lon_copy(p, d, c).start()

    def wait_sent(p, c):
        at_edge(c, lambda d: lat_copy(p, d).wait_send())
        for d in (0, 1):
            lev_copy(p, d, c).wait_send()
            lon_copy(p, d, c).wait_send()

    def wait_faces(p, c):
        at_edge(c, lambda d: lat_copy(p, d).wait_recv())
        for d in (0, 1):
            lev_copy(p, d, c).wait_recv()
            lon_copy(p, d, c).wait_recv()

    def of_line(q):
        return pl.ds(q * wide, wide)

    def cells(z):
        return pl.ds(z, wide, stride=height)

    def put(p, c, q, z, values):
        u[p, z + 1, c, of_line(q)] = values
        lon_out[p, 0, c, q * height + z] = values[0]
        lon_out[p, 1, c, q * height + z] = values[wide - 1]

    def stepped(p, c, q, z):
        i, side = q // 2, q % 2
        middle = u[p, z + 1, c, of_line(q)]
        if i == 0:
            before = u[p, z + 1, jnp.maximum(c - 1, 0), of_line(lines - 2 + side)]
            outside = jnp.where(c == 0, lat_held[side, z], before)
        else:
            outside = u[p, z + 1, c, of_line(q - 2)]
        if i == DEPTH - 1:
            end = c == chunks - 1
            at = jnp.where(end, (lines - 1 - side) * wide, side * wide)
            inside = u[
                p, z + 1, jnp.minimum(c + 1, chunks - 1), pl.ds(pl.multiple_of(at, wide), wide)
            ]
        else:
            inside = u[p, z + 1, c, of_line(q + 2)]
        low, high = u[p, z, c, of_line(q)], u[p, z + 2, c, of_line(q)]
        if z == 0:
            low = swapped(jnp.where(low_lanes, u[p, height, c, of_line(q)], low))
        if z == height - 1:
            high = swapped(jnp.where(low_lanes, high, u[p, 1, c, of_line(q)]))
        at = pl.ds(q * height + z, 1)
        west = jnp.where(first_cell, lon_in[p, 1, c, at], pltpu.roll(middle, 1, 0))
        east = jnp.where(last_cell, lon_in[p, 0, c, at], pltpu.roll(middle, wide - 1, 0))
        spread = (outside + inside) + (west + east) + (low + high) - 6.0 * middle
        return middle + ratio[z, c, of_line(q)] * spread + force[z, c, of_line(q)]

    def start_loads(c):
        for f in range(3):
            for side in (0, 1):
                load(f, c, side).start()

    barrier = pltpu.get_barrier_semaphore()
    greeted = [{"lev": partner_lev}]
    greeted += [t(d) for t in (lat_target, lev_target) for d in (0, 1)]
    greeted += [stat_target(j) for j in range(lon_size - 1)]

    def pack(f, n, c):
        slot = lax.rem(c, SLOTS)
        for q in range(lines):
            i, side = q // 2, q % 2
            row = staged(c, f, side) + (i if side == 0 else DEPTH - 1 - i)
            a, b = butterfly(final[row, cells(2 * n)], final[row, cells(2 * n + 1)])
            plane(f, 2 * n + kind)[c, of_line(q)] = jnp.where(half == 0, a, b)
            packed[slot, f, n, of_line(q)] = jnp.where(half == 0, b, a)

    def pack_all(c, meet=False):
        for f in range(3):
            for side in (0, 1):
                load(f, c, side).wait()
            for n in range(pairs):
                pack(f, n, c)
                if meet and f == 0 and n == 0:
                    pl.semaphore_wait(barrier, len(greeted))
                swap_copy(f, n, c).start()

    start_loads(0)
    for other in greeted:
        pl.semaphore_signal(barrier, inc=1, device_id=other, device_id_type=MESH)
    start_loads(1)
    pack_all(0, meet=True)
    start_loads(2)
    pack_all(1)
    start_loads(3)

    def arrange(c):
        for f in range(3):
            for n in range(pairs):
                swap_copy(f, n, c).wait_recv()
            for q in range(lines):
                for n in range(pairs):
                    at = of_line(q)
                    a, b = butterfly(plane(f, 2 * n)[c, at], plane(f, 2 * n + 1)[c, at])
                    if f == 0:
                        put(0, c, q, 2 * n, a)
                        put(0, c, q, 2 * n + 1, b)
                    else:
                        plane(f, 2 * n)[c, at] = a
                        plane(f, 2 * n + 1)[c, at] = b
            if f == 0:
                send_faces(0, c)

    def advance(s, c):
        p, q_ = (s - 1) % 2, s % 2
        if s >= 2:
            wait_sent(q_, c)
        wait_faces(p, c)

        @pl.when(c == 0)
        def _():
            lat_held[...] = lat_in[p]

        for q in range(lines):
            if s < STEPS:
                for z in range(height):
                    put(q_, c, q, z, stepped(p, c, q, z))
            else:
                for n in range(pairs):
                    a, b = butterfly(stepped(p, c, q, 2 * n), stepped(p, c, q, 2 * n + 1))
                    ratio[2 * n, c, of_line(q)] = a
                    ratio[2 * n + 1, c, of_line(q)] = b
        if s < STEPS:
            send_faces(q_, c)
        else:
            for n in range(pairs):
                back_copy(n, c).start()

    def wave(k, carry):
        @pl.when(k < chunks)
        def _():
            arrange(k)

        @pl.when(k + SLOTS < chunks)
        def _():
            c = k + SLOTS
            for f in range(3):
                for n in range(pairs):
                    swap_copy(f, n, c - SLOTS).wait_send()
            pack_all(c)

            @pl.when(c + 2 < chunks)
            def _():
                start_loads(c + 2)

        for s in range(1, STEPS + 1):

            @pl.when((k >= s) & (k < chunks + s))
            def _(s=s):
                advance(s, k - s)

        return carry

    lax.fori_loop(0, chunks + STEPS, wave, 0)

    def note(c, at, values):
        mean = jnp.sum(values, axis=0, keepdims=True) / wide
        apart = values - mean
        stat_out[c, pl.ds(at, 1)] = mean
        stat_out[c, pl.ds(at + height, 1)] = jnp.sum(apart * apart, axis=0, keepdims=True)

    def moments(c, q):
        at = pl.ds(2 * height * q, 2 * height)
        own = stat_out[c, at]
        others = [stat_in[j, c, at] for j in range(lon_size - 1)]
        summed = own
        for other in others:
            summed = summed + other
        mean = summed[:height] / lon_size
        apart = (own[:height] - mean) * (own[:height] - mean)
        for other in others:
            apart = apart + (other[:height] - mean) * (other[:height] - mean)
        variance = summed[height:] / (lon_size * wide) + apart / lon_size
        return mean, lax.rsqrt(variance + 0.0001)

    end = chunks - 1
    for q in range(lines):
        for z in range(height):
            note(end, 2 * height * q + z, ratio[z, end, of_line(q)])
    for j in range(lon_size - 1):
        stat_copy(j, end).start()

    def whole(c, q, n):
        own = ratio[2 * n + kind, c, of_line(q)]
        other = score[c * pairs + n, of_line(q)]
        return butterfly(jnp.where(half == 0, own, other), jnp.where(half == 0, other, own))

    def restore(c):
        for n in range(pairs):
            back_copy(n, c).wait_recv()
        for q in range(lines):
            row = row_of(c, q // 2, q % 2)
            for n in range(pairs):
                for z, values in zip((2 * n, 2 * n + 1), whole(c, q, n)):
                    final[row, cells(z)] = values
                    note(c, 2 * height * q + z, values)
        for j in range(lon_size - 1):
            stat_copy(j, c).start()

    def finish(c):
        for j in range(lon_size - 1):
            stat_copy(j, c).wait_recv()
        for q in range(lines):
            row = row_of(c, q // 2, q % 2)
            mean, scale = moments(c, q)
            for z in range(height):
                values = final[row, cells(z)]
                score[row, cells(z)] = (values - mean[z : z + 1]) * scale[z : z + 1]

    def share_moments():
        for j in range(lon_size - 1):
            stat_copy(j, end).wait_recv()
        for q in range(lines):
            mean, scale = moments(end, q)
            moment_out[q, pl.ds(0, height)] = mean
            moment_out[q, pl.ds(height, height)] = scale
        moment_copy.start()

    def last(c, carry):
        restore(c)
        pl.when(c > 0)(lambda: finish(c - 1))
        pl.when(c == 0)(share_moments)
        return carry

    moment_copy = remote(
        moment_out, moment_in, moment_send, moment_recv, {"lev": partner_lev}
    )
    lax.fori_loop(0, end, last, 0)
    finish(end - 1)

    moment_copy.wait_recv()

    def spread_out(own, other):
        a, b = jnp.where(half == 0, own, other), jnp.where(half == 0, other, own)
        first = lax.broadcasted_iota(jnp.int32, a.shape, 1) < members // 2
        return (
            jnp.where(first, a, pltpu.roll(b, members // 2, 1)),
            jnp.where(first, pltpu.roll(a, members // 2, 1), b),
        )

    for n in range(pairs):
        back_copy(n, end).wait_recv()
        for q in range(lines):
            row = row_of(end, q // 2, q % 2)
            for z, values in zip((2 * n, 2 * n + 1), whole(end, q, n)):
                final[row, cells(z)] = values
    for n in range(pairs):
        for q in range(lines):
            row = row_of(end, q // 2, q % 2)
            ours = 2 * n + kind
            means, scales = (
                spread_out(moment_out[q, pl.ds(o + ours, 1)], moment_in[q, pl.ds(o + ours, 1)])
                for o in (0, height)
            )
            for z, m, k in zip((2 * n, 2 * n + 1), means, scales):
                score[row, cells(z)] = (final[row, cells(z)] - m) * k

    def settle(c, carry):
        wait_sent((STEPS - 1) % 2, c)
        for n in range(pairs):
            back_copy(n, c).wait_send()
        for j in range(lon_size - 1):
            stat_copy(j, c).wait_send()
        return carry

    lax.fori_loop(0, chunks, settle, 0)
    moment_copy.wait_send()
    for c in range(chunks - SLOTS, chunks):
        for f in range(3):
            for n in range(pairs):
                swap_copy(f, n, c).wait_send()


def write_out(score, final, score_hbm, final_hbm, sem):
    rows = score.shape[0] // PARTS
    copies = [
        pltpu.make_async_copy(
            src.at[pl.ds(i * rows, rows)], dst.at[pl.ds(i * rows, rows)], sem.at[n, i]
        )
        for i in range(PARTS)
        for n, (src, dst) in enumerate(((score, score_hbm), (final, final_hbm)))
    ]
    for copy in copies:
        copy.start()
    for copy in copies:
        copy.wait()


def local(sizes, initial_heat, diffusivity_ratio, forcing_term):
    rows, wide, height, members = initial_heat.shape
    flat = (rows, wide * height, members)
    chunks, slab = rows // (2 * DEPTH), 2 * DEPTH * wide
    hbm = pl.BlockSpec(memory_space=pl.ANY)
    vmem = pl.BlockSpec(memory_space=pltpu.VMEM)
    f32, dma = jnp.float32, pltpu.SemaphoreType.DMA
    others, pairs = sizes[1] - 1, height // 2
    score, final = pl.pallas_call(
        functools.partial(kernel, sizes),
        out_shape=(pltpu.VMEM(flat, f32), pltpu.VMEM(flat, f32)),
        in_specs=[hbm, hbm, hbm],
        out_specs=(vmem, vmem),
        scratch_shapes=[
            pltpu.VMEM((2, height + 2, chunks, slab, members), f32),
            pltpu.VMEM((height, chunks, slab, members), f32),
            pltpu.VMEM((height, chunks, slab, members), f32),
            pltpu.VMEM((SLOTS, 3, pairs, slab, members), f32),
            pltpu.VMEM((2, 2, height, wide, members), f32),
            pltpu.VMEM((2, height, wide, members), f32),
            pltpu.VMEM((2, 2, chunks, 2 * DEPTH * height, members), f32),
            pltpu.VMEM((2, 2, chunks, 2 * DEPTH * height, members), f32),
            pltpu.VMEM((chunks, 4 * DEPTH * height, members), f32),
            pltpu.VMEM((others, chunks, 4 * DEPTH * height, members), f32),
            pltpu.VMEM((2 * DEPTH, 2 * height, members), f32),
            pltpu.VMEM((2 * DEPTH, 2 * height, members), f32),
            dma((3, 2, 2)),
            dma((SLOTS, 3, pairs)),
            dma((chunks, 3, pairs)),
            dma((chunks, pairs)),
            dma((chunks, pairs)),
            dma((2, 2, chunks)),
            dma((2, 2, chunks)),
            dma((2, 2, chunks)),
            dma((2, 2, chunks)),
            dma((2, 2)),
            dma((2, 2)),
            dma((others, chunks)),
            dma((others, chunks)),
            dma,
            dma,
        ],
        compiler_params=pltpu.CompilerParams(
            collective_id=0, has_side_effects=True, vmem_limit_bytes=int(47.25 * 2**20)
        ),
    )(*(a.reshape(flat) for a in (initial_heat, diffusivity_ratio, forcing_term)))
    score, final = pl.pallas_call(
        write_out,
        out_shape=(jax.ShapeDtypeStruct(flat, f32), jax.ShapeDtypeStruct(flat, f32)),
        in_specs=[vmem, vmem],
        out_specs=(hbm, hbm),
        scratch_shapes=[dma((2, PARTS))],
        compiler_params=pltpu.CompilerParams(vmem_limit_bytes=4 * 2**20),
    )(*(pltpu.with_memory_space_constraint(a, pltpu.VMEM) for a in (score, final)))
    return score.reshape(initial_heat.shape), final.reshape(initial_heat.shape)


def solution(mesh):
    sizes = tuple(mesh.shape[a] for a in ("lat", "lon", "lev"))
    placed = P("lat", "lon", "lev", None)
    return jax.shard_map(
        functools.partial(local, sizes),
        mesh=mesh,
        in_specs=(placed, placed, placed),
        out_specs=(placed, placed),
        check_vma=False,
    )
```

```python
import functools

import jax
import jax.numpy as jnp
from jax import lax
from jax.experimental import pallas as pl
from jax.experimental.pallas import tpu as pltpu
from jax.sharding import PartitionSpec as P

STEPS = 4
DEPTH = 2
SLOTS = 2
PARTS = 8
MESH = pl.DeviceIdType.MESH


def kernel(
    sizes,
    heat_hbm,
    ratio_hbm,
    force_hbm,
    score,
    final,
    u,
    ratio,
    force,
    packed,
    lat_in,
    lat_held,
    lon_out,
    lon_in,
    stat_out,
    stat_in,
    moment_out,
    moment_in,
    load_sem,
    swap_send,
    swap_recv,
    back_send,
    back_recv,
    lev_send,
    lev_recv,
    lon_send,
    lon_recv,
    lat_send,
    lat_recv,
    stat_send,
    stat_recv,
    moment_send,
    moment_recv,
    met,
):
    lat_size, lon_size, lev_size = sizes
    rows = final.shape[0]
    chunks, slab, members = u.shape[2:]
    height = u.shape[1] - 2
    pairs = height // 2
    wide = slab // (2 * DEPTH)
    lines = 2 * DEPTH
    lat, lon, lev = (lax.axis_index(a) for a in ("lat", "lon", "lev"))
    kind = lax.rem(lev, 2)
    outer_x = lat // (lat_size // 2)
    half = lax.rem(kind + outer_x, 2)
    partner_lev = lev + 1 - 2 * kind

    lane = lax.broadcasted_iota(jnp.int32, (wide, members), 1)
    line = lax.broadcasted_iota(jnp.int32, (wide, members), 0)
    low_lanes = lane < members // 2
    first_cell = line == 0
    last_cell = line == wide - 1

    def lat_target(d):
        other = lax.rem(lat + (lat_size - 1, 1)[d], lat_size)
        crossed = lax.rem(other // (lat_size // 2) + outer_x, 2)
        return {"lat": other, "lev": lev + crossed * (1 - 2 * kind)}

    def lev_target(d):
        return {"lev": lax.rem(lev + (lev_size - 2, 2)[d], lev_size)}

    def lon_target(d):
        return {"lon": lax.rem(lon + (lon_size - 1, 1)[d], lon_size)}

    def stat_target(j):
        return {"lon": lax.rem(lon + j + 1, lon_size)}

    def swapped(x):
        return pltpu.roll(x, members // 2, 1)

    def butterfly(a, b):
        return jnp.where(low_lanes, a, swapped(b)), jnp.where(low_lanes, swapped(a), b)

    def remote(src, dst, send_sem, recv_sem, target):
        return pltpu.make_async_remote_copy(
            src_ref=src,
            dst_ref=dst,
            send_sem=send_sem,
            recv_sem=recv_sem,
            device_id=target,
            device_id_type=MESH,
        )

    def row_of(c, i, side):
        return c * DEPTH + i if side == 0 else rows - 1 - c * DEPTH - i

    def staged(c, f, side):
        return (lax.rem(c, 2) * 3 + f) * lines + side * DEPTH

    def load(f, c, side):
        src = (heat_hbm, ratio_hbm, force_hbm)[f]
        first = c * DEPTH if side == 0 else rows - (c + 1) * DEPTH
        return pltpu.make_async_copy(
            src.at[pl.ds(first, DEPTH)],
            final.at[pl.ds(staged(c, f, side), DEPTH)],
            load_sem.at[f, side, lax.rem(c, 2)],
        )

    def place(z):
        return z // 2 + (z % 2) * pairs

    def planes(f, first, count):
        return (u.at[0, pl.ds(1 + first, count)], ratio.at[pl.ds(first, count)], force.at[pl.ds(first, count)])[f]

    def plane(f, n):
        return (u.at[0, 1 + n], ratio.at[n], force.at[n])[f]

    def swap_copy(f, c, at=None):
        slot = lax.rem(c, SLOTS)
        at = pl.ds(0, slab) if at is None else at
        return remote(
            packed.at[slot, f, :, at],
            planes(f, kind * pairs, pairs).at[:, c, at],
            swap_send.at[slot, f],
            swap_recv.at[c, f],
            {"lev": partner_lev},
        )

    def back_copy(c):
        return remote(
            ratio.at[pl.ds((1 - kind) * pairs, pairs), c],
            score.at[pl.ds(c * pairs, pairs)],
            back_send.at[c],
            back_recv.at[c],
            {"lev": partner_lev},
        )

    def lev_copy(p, d, c):
        src, dst = ((1, height + 1), (height, 0))[d]
        return remote(
            u.at[p, src, c],
            u.at[p, dst, c],
            lev_send.at[p, d, c],
            lev_recv.at[p, d, c],
            lev_target(d),
        )

    def lat_copy(p, d):
        return remote(
            u.at[p, pl.ds(1, height), 0, pl.ds(d * wide, wide)],
            lat_in.at[p, 1 - d],
            lat_send.at[p, d],
            lat_recv.at[p, d],
            lat_target(d),
        )

    def lon_copy(p, d, c):
        return remote(
            lon_out.at[p, d, c],
            lon_in.at[p, d, c],
            lon_send.at[p, d, c],
            lon_recv.at[p, d, c],
            lon_target(d),
        )

    def stat_copy(j, c):
        return remote(
            stat_out.at[c],
            stat_in.at[j, c],
            stat_send.at[j, c],
            stat_recv.at[j, c],
            stat_target(j),
        )

    def at_edge(c, body):
        @pl.when(c == 0)
        def _():
            for d in (0, 1):
                body(d)

    def send_faces(p, c):
        at_edge(c, lambda d: lat_copy(p, d).start())
        for d in (0, 1):
            lev_copy(p, d, c).start()
        for d in (0, 1):
            lon_copy(p, d, c).start()

    def wait_sent(p, c):
        at_edge(c, lambda d: lat_copy(p, d).wait_send())
        for d in (0, 1):
            lev_copy(p, d, c).wait_send()
            lon_copy(p, d, c).wait_send()

    def wait_faces(p, c):
        at_edge(c, lambda d: lat_copy(p, d).wait_recv())
        for d in (0, 1):
            lev_copy(p, d, c).wait_recv()
            lon_copy(p, d, c).wait_recv()

    def of_line(q):
        return pl.ds(q * wide, wide)

    def cells(z):
        return pl.ds(z, wide, stride=height)

    def put(p, c, q, z, values):
        u[p, place(z) + 1, c, of_line(q)] = values
        lon_out[p, 0, c, q * height + z] = values[0]
        lon_out[p, 1, c, q * height + z] = values[wide - 1]

    def stepped(p, c, q, z):
        i, side = q // 2, q % 2
        own = place(z) + 1
        middle = u[p, own, c, of_line(q)]
        if i == 0:
            before = u[p, own, jnp.maximum(c - 1, 0), of_line(lines - 2 + side)]
            outside = jnp.where(c == 0, lat_held[side, place(z)], before)
        else:
            outside = u[p, own, c, of_line(q - 2)]
        if i == DEPTH - 1:
            end = c == chunks - 1
            at = jnp.where(end, (lines - 1 - side) * wide, side * wide)
            inside = u[
                p, own, jnp.minimum(c + 1, chunks - 1), pl.ds(pl.multiple_of(at, wide), wide)
            ]
        else:
            inside = u[p, own, c, of_line(q + 2)]
        bottom, top = u[p, 1, c, of_line(q)], u[p, height, c, of_line(q)]
        if z == 0:
            low = swapped(jnp.where(low_lanes, top, u[p, 0, c, of_line(q)]))
        else:
            low = u[p, place(z - 1) + 1, c, of_line(q)]
        if z == height - 1:
            high = swapped(jnp.where(low_lanes, u[p, height + 1, c, of_line(q)], bottom))
        else:
            high = u[p, place(z + 1) + 1, c, of_line(q)]
        at = pl.ds(q * height + z, 1)
        west = jnp.where(first_cell, lon_in[p, 1, c, at], pltpu.roll(middle, 1, 0))
        east = jnp.where(last_cell, lon_in[p, 0, c, at], pltpu.roll(middle, wide - 1, 0))
        spread = (outside + inside) + (west + east) + (low + high) - 6.0 * middle
        return middle + ratio[own - 1, c, of_line(q)] * spread + force[own - 1, c, of_line(q)]

    def start_loads(c):
        for f in range(3):
            for side in (0, 1):
                load(f, c, side).start()

    barrier = pltpu.get_barrier_semaphore()
    second = lev - kind + 1
    near = [{**lat_target(d), "lev": second} for d in (0, 1)]
    near += [{"lev": lax.rem(second + move, lev_size)} for move in (2, lev_size - 2)]
    near += [{**stat_target(j), "lev": second} for j in range(lon_size - 1)]
    partner = {"lev": partner_lev}

    def signal(sem, other):
        pl.semaphore_signal(sem, inc=1, device_id=other, device_id_type=MESH)

    def meet_partner():
        @pl.when(kind == 0)
        def _():
            pl.semaphore_wait(barrier, 1)
            signal(met, partner)

        @pl.when(kind == 1)
        def _():
            pl.semaphore_wait(met, 1)

    def meet_all():
        @pl.when(kind == 1)
        def _():
            pl.semaphore_wait(barrier, 1 + 2 * len(near))
            signal(met, partner)

        @pl.when(kind == 0)
        def _():
            pl.semaphore_wait(met, 1)

    def pack(f, q, c):
        slot = lax.rem(c, SLOTS)
        i, side = q // 2, q % 2
        row = staged(c, f, side) + (i if side == 0 else DEPTH - 1 - i)
        for n in range(pairs):
            a, b = butterfly(final[row, cells(2 * n)], final[row, cells(2 * n + 1)])
            plane(f, kind * pairs + n)[c, of_line(q)] = jnp.where(half == 0, a, b)
            packed[slot, f, n, of_line(q)] = jnp.where(half == 0, b, a)

    def pack_all(c, meet=False):
        for f in range(3):
            for side in (0, 1):
                load(f, c, side).wait()
                for i in range(DEPTH):
                    q = 2 * i + side
                    pack(f, q, c)
                    if meet and f == 0:
                        if q == 0:
                            meet_partner()
                        swap_copy(f, c, of_line(q)).start()
            if not (meet and f == 0):
                swap_copy(f, c).start()

    start_loads(0)
    for other in [partner, *near]:
        signal(barrier, other)
    start_loads(1)
    pack_all(0, meet=True)
    start_loads(2)
    pack_all(1)
    start_loads(3)
    meet_all()

    def arrange(c):
        for f in range(3):
            swap_copy(f, c).wait_recv()
            for q in range(lines):
                for n in range(pairs):
                    at = of_line(q)
                    a, b = butterfly(plane(f, n)[c, at], plane(f, pairs + n)[c, at])
                    if f == 0:
                        put(0, c, q, 2 * n, a)
                        put(0, c, q, 2 * n + 1, b)
                    else:
                        plane(f, n)[c, at] = a
                        plane(f, pairs + n)[c, at] = b
            if f == 0:
                send_faces(0, c)

    def advance(s, c):
        p, q_ = (s - 1) % 2, s % 2
        if s >= 2:
            wait_sent(q_, c)
        wait_faces(p, c)

        @pl.when(c == 0)
        def _():
            lat_held[...] = lat_in[p]

        for q in range(lines):
            if s < STEPS:
                for z in range(height):
                    put(q_, c, q, z, stepped(p, c, q, z))
            else:
                for n in range(pairs):
                    a, b = butterfly(stepped(p, c, q, 2 * n), stepped(p, c, q, 2 * n + 1))
                    ratio[n, c, of_line(q)] = a
                    ratio[pairs + n, c, of_line(q)] = b
        if s < STEPS:
            send_faces(q_, c)
        else:
            back_copy(c).start()

    def wave(k, carry):
        @pl.when(k < chunks)
        def _():
            arrange(k)

        @pl.when(k + SLOTS < chunks)
        def _():
            c = k + SLOTS
            for f in range(3):
                swap_copy(f, c - SLOTS).wait_send()
            pack_all(c)

            @pl.when(c + 2 < chunks)
            def _():
                start_loads(c + 2)

        for s in range(1, STEPS + 1):

            @pl.when((k >= s) & (k < chunks + s))
            def _(s=s):
                advance(s, k - s)

        return carry

    lax.fori_loop(0, chunks + STEPS, wave, 0)

    def note(c, at, values):
        mean = jnp.sum(values, axis=0, keepdims=True) / wide
        apart = values - mean
        stat_out[c, pl.ds(at, 1)] = mean
        stat_out[c, pl.ds(at + height, 1)] = jnp.sum(apart * apart, axis=0, keepdims=True)

    def moments(c, q):
        at = pl.ds(2 * height * q, 2 * height)
        own = stat_out[c, at]
        others = [stat_in[j, c, at] for j in range(lon_size - 1)]
        summed = own
        for other in others:
            summed = summed + other
        mean = summed[:height] / lon_size
        apart = (own[:height] - mean) * (own[:height] - mean)
        for other in others:
            apart = apart + (other[:height] - mean) * (other[:height] - mean)
        variance = summed[height:] / (lon_size * wide) + apart / lon_size
        return mean, lax.rsqrt(variance + 0.0001)

    end = chunks - 1
    for q in range(lines):
        for z in range(height):
            note(end, 2 * height * q + z, ratio[z, end, of_line(q)])
    for j in range(lon_size - 1):
        stat_copy(j, end).start()

    def whole(c, q, n):
        own = ratio[kind * pairs + n, c, of_line(q)]
        other = score[c * pairs + n, of_line(q)]
        return butterfly(jnp.where(half == 0, own, other), jnp.where(half == 0, other, own))

    def restore(c):
        back_copy(c).wait_recv()
        for q in range(lines):
            row = row_of(c, q // 2, q % 2)
            for n in range(pairs):
                for z, values in zip((2 * n, 2 * n + 1), whole(c, q, n)):
                    final[row, cells(z)] = values
                    note(c, 2 * height * q + z, values)
        for j in range(lon_size - 1):
            stat_copy(j, c).start()

    def finish(c):
        for j in range(lon_size - 1):
            stat_copy(j, c).wait_recv()
        for q in range(lines):
            row = row_of(c, q // 2, q % 2)
            mean, scale = moments(c, q)
            for z in range(height):
                values = final[row, cells(z)]
                score[row, cells(z)] = (values - mean[z : z + 1]) * scale[z : z + 1]

    def share_moments():
        for j in range(lon_size - 1):
            stat_copy(j, end).wait_recv()
        for q in range(lines):
            mean, scale = moments(end, q)
            moment_out[q, pl.ds(0, height)] = mean
            moment_out[q, pl.ds(height, height)] = scale
        moment_copy.start()

    def last(c, carry):
        restore(c)
        pl.when(c > 0)(lambda: finish(c - 1))
        pl.when(c == 0)(share_moments)
        return carry

    moment_copy = remote(
        moment_out, moment_in, moment_send, moment_recv, {"lev": partner_lev}
    )
    lax.fori_loop(0, end, last, 0)
    finish(end - 1)

    moment_copy.wait_recv()

    def spread_out(own, other):
        a, b = jnp.where(half == 0, own, other), jnp.where(half == 0, other, own)
        first = lax.broadcasted_iota(jnp.int32, a.shape, 1) < members // 2
        return (
            jnp.where(first, a, pltpu.roll(b, members // 2, 1)),
            jnp.where(first, pltpu.roll(a, members // 2, 1), b),
        )

    back_copy(end).wait_recv()
    for n in range(pairs):
        for q in range(lines):
            row = row_of(end, q // 2, q % 2)
            for z, values in zip((2 * n, 2 * n + 1), whole(end, q, n)):
                final[row, cells(z)] = values
    for n in range(pairs):
        for q in range(lines):
            row = row_of(end, q // 2, q % 2)
            ours = kind * pairs + n
            means, scales = (
                spread_out(moment_out[q, pl.ds(o + ours, 1)], moment_in[q, pl.ds(o + ours, 1)])
                for o in (0, height)
            )
            for z, m, k in zip((2 * n, 2 * n + 1), means, scales):
                score[row, cells(z)] = (final[row, cells(z)] - m) * k

    def settle(c, carry):
        wait_sent((STEPS - 1) % 2, c)
        back_copy(c).wait_send()
        for j in range(lon_size - 1):
            stat_copy(j, c).wait_send()
        return carry

    lax.fori_loop(0, chunks, settle, 0)
    moment_copy.wait_send()
    for c in range(chunks - SLOTS, chunks):
        for f in range(3):
            swap_copy(f, c).wait_send()


def write_out(score, final, score_hbm, final_hbm, sem):
    rows = score.shape[0] // PARTS
    copies = [
        pltpu.make_async_copy(
            src.at[pl.ds(i * rows, rows)], dst.at[pl.ds(i * rows, rows)], sem.at[n, i]
        )
        for i in range(PARTS)
        for n, (src, dst) in enumerate(((score, score_hbm), (final, final_hbm)))
    ]
    for copy in copies:
        copy.start()
    for copy in copies:
        copy.wait()


def local(sizes, initial_heat, diffusivity_ratio, forcing_term):
    rows, wide, height, members = initial_heat.shape
    flat = (rows, wide * height, members)
    chunks, slab = rows // (2 * DEPTH), 2 * DEPTH * wide
    hbm = pl.BlockSpec(memory_space=pl.ANY)
    vmem = pl.BlockSpec(memory_space=pltpu.VMEM)
    f32, dma = jnp.float32, pltpu.SemaphoreType.DMA
    others, pairs = sizes[1] - 1, height // 2
    score, final = pl.pallas_call(
        functools.partial(kernel, sizes),
        out_shape=(pltpu.VMEM(flat, f32), pltpu.VMEM(flat, f32)),
        in_specs=[hbm, hbm, hbm],
        out_specs=(vmem, vmem),
        scratch_shapes=[
            pltpu.VMEM((2, height + 2, chunks, slab, members), f32),
            pltpu.VMEM((height, chunks, slab, members), f32),
            pltpu.VMEM((height, chunks, slab, members), f32),
            pltpu.VMEM((SLOTS, 3, pairs, slab, members), f32),
            pltpu.VMEM((2, 2, height, wide, members), f32),
            pltpu.VMEM((2, height, wide, members), f32),
            pltpu.VMEM((2, 2, chunks, 2 * DEPTH * height, members), f32),
            pltpu.VMEM((2, 2, chunks, 2 * DEPTH * height, members), f32),
            pltpu.VMEM((chunks, 4 * DEPTH * height, members), f32),
            pltpu.VMEM((others, chunks, 4 * DEPTH * height, members), f32),
            pltpu.VMEM((2 * DEPTH, 2 * height, members), f32),
            pltpu.VMEM((2 * DEPTH, 2 * height, members), f32),
            dma((3, 2, 2)),
            dma((SLOTS, 3)),
            dma((chunks, 3)),
            dma((chunks,)),
            dma((chunks,)),
            dma((2, 2, chunks)),
            dma((2, 2, chunks)),
            dma((2, 2, chunks)),
            dma((2, 2, chunks)),
            dma((2, 2)),
            dma((2, 2)),
            dma((others, chunks)),
            dma((others, chunks)),
            dma,
            dma,
            pltpu.SemaphoreType.REGULAR,
        ],
        compiler_params=pltpu.CompilerParams(
            collective_id=0, has_side_effects=True, vmem_limit_bytes=int(47.25 * 2**20)
        ),
    )(*(a.reshape(flat) for a in (initial_heat, diffusivity_ratio, forcing_term)))
    score, final = pl.pallas_call(
        write_out,
        out_shape=(jax.ShapeDtypeStruct(flat, f32), jax.ShapeDtypeStruct(flat, f32)),
        in_specs=[vmem, vmem],
        out_specs=(hbm, hbm),
        scratch_shapes=[dma((2, PARTS))],
        compiler_params=pltpu.CompilerParams(vmem_limit_bytes=4 * 2**20),
    )(*(pltpu.with_memory_space_constraint(a, pltpu.VMEM) for a in (score, final)))
    return score.reshape(initial_heat.shape), final.reshape(initial_heat.shape)


def solution(mesh):
    sizes = tuple(mesh.shape[a] for a in ("lat", "lon", "lev"))
    placed = P("lat", "lon", "lev", None)
    return jax.shard_map(
        functools.partial(local, sizes),
        mesh=mesh,
        in_specs=(placed, placed, placed),
        out_specs=(placed, placed),
        check_vma=False,
    )
```

```python
import functools

import jax
import jax.numpy as jnp
from jax import lax
from jax.experimental import pallas as pl
from jax.experimental.pallas import tpu as pltpu
from jax.sharding import PartitionSpec as P

STEPS = 4
DEPTH = 2
SLOTS = 2
PARTS = 8
MESH = pl.DeviceIdType.MESH


def kernel(
    sizes,
    heat_hbm,
    ratio_hbm,
    force_hbm,
    score,
    final,
    u,
    ratio,
    force,
    packed,
    lat_in,
    lat_held,
    lon_out,
    lon_in,
    stat_out,
    stat_in,
    moment_out,
    moment_in,
    load_sem,
    swap_send,
    swap_recv,
    back_send,
    back_recv,
    lev_send,
    lev_recv,
    lon_send,
    lon_recv,
    lat_send,
    lat_recv,
    stat_send,
    stat_recv,
    moment_send,
    moment_recv,
    met,
):
    lat_size, lon_size, lev_size = sizes
    rows = final.shape[0]
    chunks, slab, members = u.shape[2:]
    height = u.shape[1] - 2
    pairs = height // 2
    wide = slab // (2 * DEPTH)
    lines = 2 * DEPTH
    lat, lon, lev = (lax.axis_index(a) for a in ("lat", "lon", "lev"))
    kind = lax.rem(lev, 2)
    outer_x = lat // (lat_size // 2)
    half = lax.rem(kind + outer_x, 2)
    partner_lev = lev + 1 - 2 * kind

    lane = lax.broadcasted_iota(jnp.int32, (wide, members), 1)
    line = lax.broadcasted_iota(jnp.int32, (wide, members), 0)
    low_lanes = lane < members // 2
    first_cell = line == 0
    last_cell = line == wide - 1

    def lat_target(d):
        other = lax.rem(lat + (lat_size - 1, 1)[d], lat_size)
        crossed = lax.rem(other // (lat_size // 2) + outer_x, 2)
        return {"lat": other, "lev": lev + crossed * (1 - 2 * kind)}

    def lev_target(d):
        return {"lev": lax.rem(lev + (lev_size - 2, 2)[d], lev_size)}

    def lon_target(d):
        return {"lon": lax.rem(lon + (lon_size - 1, 1)[d], lon_size)}

    def stat_target(j):
        return {"lon": lax.rem(lon + j + 1, lon_size)}

    def swapped(x):
        return pltpu.roll(x, members // 2, 1)

    def butterfly(a, b):
        return jnp.where(low_lanes, a, swapped(b)), jnp.where(low_lanes, swapped(a), b)

    def remote(src, dst, send_sem, recv_sem, target):
        return pltpu.make_async_remote_copy(
            src_ref=src,
            dst_ref=dst,
            send_sem=send_sem,
            recv_sem=recv_sem,
            device_id=target,
            device_id_type=MESH,
        )

    def row_of(c, i, side):
        return c * DEPTH + i if side == 0 else rows - 1 - c * DEPTH - i

    def staged(c, f, side):
        return (lax.rem(c, 2) * 3 + f) * lines + side * DEPTH

    def load(f, c, side):
        src = (heat_hbm, ratio_hbm, force_hbm)[f]
        first = c * DEPTH if side == 0 else rows - (c + 1) * DEPTH
        return pltpu.make_async_copy(
            src.at[pl.ds(first, DEPTH)],
            final.at[pl.ds(staged(c, f, side), DEPTH)],
            load_sem.at[f, side, lax.rem(c, 2)],
        )

    def place(z):
        return z // 2 + (z % 2) * pairs

    def planes(f, first, count):
        return (u.at[0, pl.ds(1 + first, count)], ratio.at[pl.ds(first, count)], force.at[pl.ds(first, count)])[f]

    def plane(f, n):
        return (u.at[0, 1 + n], ratio.at[n], force.at[n])[f]

    def swap_copy(f, c, at=None):
        slot = lax.rem(c, SLOTS)
        at = pl.ds(0, slab) if at is None else at
        return remote(
            packed.at[slot, f, :, at],
            planes(f, kind * pairs, pairs).at[:, c, at],
            swap_send.at[slot, f],
            swap_recv.at[c, f],
            {"lev": partner_lev},
        )

    def back_copy(c, q=None):
        at = pl.ds(0, slab) if q is None else pl.ds(q * wide, wide)
        return remote(
            ratio.at[pl.ds((1 - kind) * pairs, pairs), c, at],
            score.at[pl.ds(c * pairs, pairs), at],
            back_send.at[c],
            back_recv.at[c if q is None else chunks + q],
            {"lev": partner_lev},
        )

    last_lines = [q for side in (1, 0) for q in range(side, lines, 2)]

    def lev_copy(p, d, c):
        src, dst = ((1, height + 1), (height, 0))[d]
        return remote(
            u.at[p, src, c],
            u.at[p, dst, c],
            lev_send.at[p, d, c],
            lev_recv.at[p, d, c],
            lev_target(d),
        )

    def lat_copy(p, d):
        return remote(
            u.at[p, pl.ds(1, height), 0, pl.ds(d * wide, wide)],
            lat_in.at[p, 1 - d],
            lat_send.at[p, d],
            lat_recv.at[p, d],
            lat_target(d),
        )

    def lon_copy(p, d, c):
        return remote(
            lon_out.at[p, d, c],
            lon_in.at[p, d, c],
            lon_send.at[p, d, c],
            lon_recv.at[p, d, c],
            lon_target(d),
        )

    def stat_copy(j, c):
        return remote(
            stat_out.at[c],
            stat_in.at[j, c],
            stat_send.at[j, c],
            stat_recv.at[j, c],
            stat_target(j),
        )

    def at_edge(c, body):
        @pl.when(c == 0)
        def _():
            for d in (0, 1):
                body(d)

    def send_faces(p, c):
        at_edge(c, lambda d: lat_copy(p, d).start())
        for d in (0, 1):
            lev_copy(p, d, c).start()
        for d in (0, 1):
            lon_copy(p, d, c).start()

    def wait_sent(p, c):
        at_edge(c, lambda d: lat_copy(p, d).wait_send())
        for d in (0, 1):
            lev_copy(p, d, c).wait_send()
            lon_copy(p, d, c).wait_send()

    def wait_faces(p, c):
        at_edge(c, lambda d: lat_copy(p, d).wait_recv())
        for d in (0, 1):
            lev_copy(p, d, c).wait_recv()
            lon_copy(p, d, c).wait_recv()

    def of_line(q):
        return pl.ds(q * wide, wide)

    def cells(z):
        return pl.ds(z, wide, stride=height)

    def put(p, c, q, z, values):
        u[p, place(z) + 1, c, of_line(q)] = values
        lon_out[p, 0, c, q * height + z] = values[0]
        lon_out[p, 1, c, q * height + z] = values[wide - 1]

    def stepped(p, c, q, z):
        i, side = q // 2, q % 2
        own = place(z) + 1
        middle = u[p, own, c, of_line(q)]
        if i == 0:
            before = u[p, own, jnp.maximum(c - 1, 0), of_line(lines - 2 + side)]
            outside = jnp.where(c == 0, lat_held[side, place(z)], before)
        else:
            outside = u[p, own, c, of_line(q - 2)]
        if i == DEPTH - 1:
            end = c == chunks - 1
            at = jnp.where(end, (lines - 1 - side) * wide, side * wide)
            inside = u[
                p, own, jnp.minimum(c + 1, chunks - 1), pl.ds(pl.multiple_of(at, wide), wide)
            ]
        else:
            inside = u[p, own, c, of_line(q + 2)]
        bottom, top = u[p, 1, c, of_line(q)], u[p, height, c, of_line(q)]
        if z == 0:
            low = swapped(jnp.where(low_lanes, top, u[p, 0, c, of_line(q)]))
        else:
            low = u[p, place(z - 1) + 1, c, of_line(q)]
        if z == height - 1:
            high = swapped(jnp.where(low_lanes, u[p, height + 1, c, of_line(q)], bottom))
        else:
            high = u[p, place(z + 1) + 1, c, of_line(q)]
        at = pl.ds(q * height + z, 1)
        west = jnp.where(first_cell, lon_in[p, 1, c, at], pltpu.roll(middle, 1, 0))
        east = jnp.where(last_cell, lon_in[p, 0, c, at], pltpu.roll(middle, wide - 1, 0))
        spread = (outside + inside) + (west + east) + (low + high) - 6.0 * middle
        return middle + ratio[own - 1, c, of_line(q)] * spread + force[own - 1, c, of_line(q)]

    def start_loads(c):
        for f in range(3):
            for side in (0, 1):
                load(f, c, side).start()

    barrier = pltpu.get_barrier_semaphore()
    second = lev - kind + 1
    near = [{**lat_target(d), "lev": second} for d in (0, 1)]
    near += [{"lev": lax.rem(second + move, lev_size)} for move in (2, lev_size - 2)]
    near += [{**stat_target(j), "lev": second} for j in range(lon_size - 1)]
    partner = {"lev": partner_lev}

    def signal(sem, other):
        pl.semaphore_signal(sem, inc=1, device_id=other, device_id_type=MESH)

    def meet_partner():
        @pl.when(kind == 0)
        def _():
            pl.semaphore_wait(barrier, 1)
            signal(met, partner)

        @pl.when(kind == 1)
        def _():
            pl.semaphore_wait(met, 1)

    def meet_all():
        @pl.when(kind == 1)
        def _():
            pl.semaphore_wait(barrier, 1 + 2 * len(near))
            signal(met, partner)

        @pl.when(kind == 0)
        def _():
            pl.semaphore_wait(met, 1)

    def pack(f, q, c):
        slot = lax.rem(c, SLOTS)
        i, side = q // 2, q % 2
        row = staged(c, f, side) + (i if side == 0 else DEPTH - 1 - i)
        for n in range(pairs):
            a, b = butterfly(final[row, cells(2 * n)], final[row, cells(2 * n + 1)])
            plane(f, kind * pairs + n)[c, of_line(q)] = jnp.where(half == 0, a, b)
            packed[slot, f, n, of_line(q)] = jnp.where(half == 0, b, a)

    def pack_all(c, meet=False):
        for f in range(3):
            for side in (0, 1):
                load(f, c, side).wait()
                for i in range(DEPTH):
                    q = 2 * i + side
                    pack(f, q, c)
                    if meet and f == 0:
                        if q == 0:
                            meet_partner()
                        swap_copy(f, c, of_line(q)).start()
            if not (meet and f == 0):
                swap_copy(f, c).start()

    start_loads(0)
    for other in [partner, *near]:
        signal(barrier, other)
    start_loads(1)
    pack_all(0, meet=True)
    start_loads(2)
    pack_all(1)
    start_loads(3)
    meet_all()

    def arrange(c):
        for f in range(3):
            swap_copy(f, c).wait_recv()
            for q in range(lines):
                for n in range(pairs):
                    at = of_line(q)
                    a, b = butterfly(plane(f, n)[c, at], plane(f, pairs + n)[c, at])
                    if f == 0:
                        put(0, c, q, 2 * n, a)
                        put(0, c, q, 2 * n + 1, b)
                    else:
                        plane(f, n)[c, at] = a
                        plane(f, pairs + n)[c, at] = b
            if f == 0:
                send_faces(0, c)

    def advance(s, c):
        p, q_ = (s - 1) % 2, s % 2
        if s >= 2:
            wait_sent(q_, c)
        wait_faces(p, c)

        @pl.when(c == 0)
        def _():
            lat_held[...] = lat_in[p]

        for q in range(lines):
            if s < STEPS:
                for z in range(height):
                    put(q_, c, q, z, stepped(p, c, q, z))
            else:
                for n in range(pairs):
                    a, b = butterfly(stepped(p, c, q, 2 * n), stepped(p, c, q, 2 * n + 1))
                    ratio[n, c, of_line(q)] = a
                    ratio[pairs + n, c, of_line(q)] = b
        if s < STEPS:
            send_faces(q_, c)
        else:

            @pl.when(c < chunks - 1)
            def _():
                back_copy(c).start()

            @pl.when(c == chunks - 1)
            def _():
                for q in last_lines:
                    back_copy(chunks - 1, q).start()

    def wave(k, carry):
        @pl.when(k < chunks)
        def _():
            arrange(k)

        @pl.when(k + SLOTS < chunks)
        def _():
            c = k + SLOTS
            for f in range(3):
                swap_copy(f, c - SLOTS).wait_send()
            pack_all(c)

            @pl.when(c + 2 < chunks)
            def _():
                start_loads(c + 2)

        for s in range(1, STEPS + 1):

            @pl.when((k >= s) & (k < chunks + s))
            def _(s=s):
                advance(s, k - s)

        return carry

    lax.fori_loop(0, chunks + STEPS, wave, 0)

    def note(c, at, values):
        mean = jnp.sum(values, axis=0, keepdims=True) / wide
        apart = values - mean
        stat_out[c, pl.ds(at, 1)] = mean
        stat_out[c, pl.ds(at + height, 1)] = jnp.sum(apart * apart, axis=0, keepdims=True)

    def moments(c, q):
        at = pl.ds(2 * height * q, 2 * height)
        own = stat_out[c, at]
        others = [stat_in[j, c, at] for j in range(lon_size - 1)]
        summed = own
        for other in others:
            summed = summed + other
        mean = summed[:height] / lon_size
        apart = (own[:height] - mean) * (own[:height] - mean)
        for other in others:
            apart = apart + (other[:height] - mean) * (other[:height] - mean)
        variance = summed[height:] / (lon_size * wide) + apart / lon_size
        return mean, lax.rsqrt(variance + 0.0001)

    end = chunks - 1
    for q in range(lines):
        for z in range(height):
            note(end, 2 * height * q + z, ratio[z, end, of_line(q)])
    for j in range(lon_size - 1):
        stat_copy(j, end).start()

    def whole(c, q, n):
        own = ratio[kind * pairs + n, c, of_line(q)]
        other = score[c * pairs + n, of_line(q)]
        return butterfly(jnp.where(half == 0, own, other), jnp.where(half == 0, other, own))

    def restore(c):
        back_copy(c).wait_recv()
        for q in range(lines):
            row = row_of(c, q // 2, q % 2)
            for n in range(pairs):
                for z, values in zip((2 * n, 2 * n + 1), whole(c, q, n)):
                    final[row, cells(z)] = values
                    note(c, 2 * height * q + z, values)
        for j in range(lon_size - 1):
            stat_copy(j, c).start()

    def finish(c):
        for j in range(lon_size - 1):
            stat_copy(j, c).wait_recv()
        for q in range(lines):
            row = row_of(c, q // 2, q % 2)
            mean, scale = moments(c, q)
            for z in range(height):
                values = final[row, cells(z)]
                score[row, cells(z)] = (values - mean[z : z + 1]) * scale[z : z + 1]

    def share_moments():
        for j in range(lon_size - 1):
            stat_copy(j, end).wait_recv()
        for q in range(lines):
            mean, scale = moments(end, q)
            moment_out[q, pl.ds(0, height)] = mean
            moment_out[q, pl.ds(height, height)] = scale
        moment_copy.start()

    def last(c, carry):
        restore(c)
        pl.when(c > 0)(lambda: finish(c - 1))
        pl.when(c == 0)(share_moments)
        return carry

    moment_copy = remote(
        moment_out, moment_in, moment_send, moment_recv, {"lev": partner_lev}
    )
    lax.fori_loop(0, end, last, 0)
    finish(end - 1)

    moment_copy.wait_recv()

    def spread_out(own, other):
        a, b = jnp.where(half == 0, own, other), jnp.where(half == 0, other, own)
        first = lax.broadcasted_iota(jnp.int32, a.shape, 1) < members // 2
        return (
            jnp.where(first, a, pltpu.roll(b, members // 2, 1)),
            jnp.where(first, pltpu.roll(a, members // 2, 1), b),
        )

    def bring(q):
        back_copy(end, q).wait_recv()
        row = row_of(end, q // 2, q % 2)
        for n in range(pairs):
            for z, values in zip((2 * n, 2 * n + 1), whole(end, q, n)):
                final[row, cells(z)] = values

    def rate(q):
        row = row_of(end, q // 2, q % 2)
        for n in range(pairs):
            ours = kind * pairs + n
            means, scales = (
                spread_out(moment_out[q, pl.ds(o + ours, 1)], moment_in[q, pl.ds(o + ours, 1)])
                for o in (0, height)
            )
            for z, m, k in zip((2 * n, 2 * n + 1), means, scales):
                score[row, cells(z)] = (final[row, cells(z)] - m) * k

    for q in last_lines[:DEPTH]:
        bring(q)
        rate(q)
    for q in last_lines[DEPTH:]:
        bring(q)
    for q in last_lines[DEPTH:]:
        rate(q)

    def settle(c, carry):
        wait_sent((STEPS - 1) % 2, c)
        back_copy(c).wait_send()
        for j in range(lon_size - 1):
            stat_copy(j, c).wait_send()
        return carry

    lax.fori_loop(0, chunks, settle, 0)
    moment_copy.wait_send()
    for c in range(chunks - SLOTS, chunks):
        for f in range(3):
            swap_copy(f, c).wait_send()


def write_out(score, final, score_hbm, final_hbm, sem):
    rows = score.shape[0] // PARTS
    copies = [
        pltpu.make_async_copy(
            src.at[pl.ds(i * rows, rows)], dst.at[pl.ds(i * rows, rows)], sem.at[n, i]
        )
        for i in range(PARTS)
        for n, (src, dst) in enumerate(((score, score_hbm), (final, final_hbm)))
    ]
    for copy in copies:
        copy.start()
    for copy in copies:
        copy.wait()


def local(sizes, initial_heat, diffusivity_ratio, forcing_term):
    rows, wide, height, members = initial_heat.shape
    flat = (rows, wide * height, members)
    chunks, slab = rows // (2 * DEPTH), 2 * DEPTH * wide
    hbm = pl.BlockSpec(memory_space=pl.ANY)
    vmem = pl.BlockSpec(memory_space=pltpu.VMEM)
    f32, dma = jnp.float32, pltpu.SemaphoreType.DMA
    others, pairs = sizes[1] - 1, height // 2
    score, final = pl.pallas_call(
        functools.partial(kernel, sizes),
        out_shape=(pltpu.VMEM(flat, f32), pltpu.VMEM(flat, f32)),
        in_specs=[hbm, hbm, hbm],
        out_specs=(vmem, vmem),
        scratch_shapes=[
            pltpu.VMEM((2, height + 2, chunks, slab, members), f32),
            pltpu.VMEM((height, chunks, slab, members), f32),
            pltpu.VMEM((height, chunks, slab, members), f32),
            pltpu.VMEM((SLOTS, 3, pairs, slab, members), f32),
            pltpu.VMEM((2, 2, height, wide, members), f32),
            pltpu.VMEM((2, height, wide, members), f32),
            pltpu.VMEM((2, 2, chunks, 2 * DEPTH * height, members), f32),
            pltpu.VMEM((2, 2, chunks, 2 * DEPTH * height, members), f32),
            pltpu.VMEM((chunks, 4 * DEPTH * height, members), f32),
            pltpu.VMEM((others, chunks, 4 * DEPTH * height, members), f32),
            pltpu.VMEM((2 * DEPTH, 2 * height, members), f32),
            pltpu.VMEM((2 * DEPTH, 2 * height, members), f32),
            dma((3, 2, 2)),
            dma((SLOTS, 3)),
            dma((chunks, 3)),
            dma((chunks,)),
            dma((chunks + 2 * DEPTH,)),
            dma((2, 2, chunks)),
            dma((2, 2, chunks)),
            dma((2, 2, chunks)),
            dma((2, 2, chunks)),
            dma((2, 2)),
            dma((2, 2)),
            dma((others, chunks)),
            dma((others, chunks)),
            dma,
            dma,
            pltpu.SemaphoreType.REGULAR,
        ],
        compiler_params=pltpu.CompilerParams(
            collective_id=0, has_side_effects=True, vmem_limit_bytes=int(47.25 * 2**20)
        ),
    )(*(a.reshape(flat) for a in (initial_heat, diffusivity_ratio, forcing_term)))
    score, final = pl.pallas_call(
        write_out,
        out_shape=(jax.ShapeDtypeStruct(flat, f32), jax.ShapeDtypeStruct(flat, f32)),
        in_specs=[vmem, vmem],
        out_specs=(hbm, hbm),
        scratch_shapes=[dma((2, PARTS))],
        compiler_params=pltpu.CompilerParams(vmem_limit_bytes=4 * 2**20),
    )(*(pltpu.with_memory_space_constraint(a, pltpu.VMEM) for a in (score, final)))
    return score.reshape(initial_heat.shape), final.reshape(initial_heat.shape)


def solution(mesh):
    sizes = tuple(mesh.shape[a] for a in ("lat", "lon", "lev"))
    placed = P("lat", "lon", "lev", None)
    return jax.shard_map(
        functools.partial(local, sizes),
        mesh=mesh,
        in_specs=(placed, placed, placed),
        out_specs=(placed, placed),
        check_vma=False,
    )
```

```python
import functools

import jax
import jax.numpy as jnp
from jax import lax
from jax.experimental import pallas as pl
from jax.experimental.pallas import tpu as pltpu
from jax.sharding import PartitionSpec as P

STEPS = 4
DEPTH = 2
SLOTS = 2
PARTS = 16
MESH = pl.DeviceIdType.MESH


def kernel(
    sizes,
    heat_hbm,
    ratio_hbm,
    force_hbm,
    score,
    final,
    u,
    ratio,
    force,
    packed,
    lat_in,
    lat_held,
    lon_out,
    lon_in,
    stat_out,
    stat_in,
    moment_out,
    moment_in,
    load_sem,
    swap_send,
    swap_recv,
    back_send,
    back_recv,
    lev_send,
    lev_recv,
    lon_send,
    lon_recv,
    lat_send,
    lat_recv,
    stat_send,
    stat_recv,
    moment_send,
    moment_recv,
    met,
):
    lat_size, lon_size, lev_size = sizes
    rows = final.shape[0]
    chunks, slab, members = u.shape[2:]
    height = u.shape[1] - 2
    pairs = height // 2
    wide = slab // (2 * DEPTH)
    lines = 2 * DEPTH
    lat, lon, lev = (lax.axis_index(a) for a in ("lat", "lon", "lev"))
    kind = lax.rem(lev, 2)
    outer_x = lat // (lat_size // 2)
    half = lax.rem(kind + outer_x, 2)
    partner_lev = lev + 1 - 2 * kind

    lane = lax.broadcasted_iota(jnp.int32, (wide, members), 1)
    line = lax.broadcasted_iota(jnp.int32, (wide, members), 0)
    low_lanes = lane < members // 2
    first_cell = line == 0
    last_cell = line == wide - 1

    def lat_target(d):
        other = lax.rem(lat + (lat_size - 1, 1)[d], lat_size)
        crossed = lax.rem(other // (lat_size // 2) + outer_x, 2)
        return {"lat": other, "lev": lev + crossed * (1 - 2 * kind)}

    def lev_target(d):
        return {"lev": lax.rem(lev + (lev_size - 2, 2)[d], lev_size)}

    def lon_target(d):
        return {"lon": lax.rem(lon + (lon_size - 1, 1)[d], lon_size)}

    def stat_target(j):
        return {"lon": lax.rem(lon + j + 1, lon_size)}

    def swapped(x):
        return pltpu.roll(x, members // 2, 1)

    def butterfly(a, b):
        return jnp.where(low_lanes, a, swapped(b)), jnp.where(low_lanes, swapped(a), b)

    def remote(src, dst, send_sem, recv_sem, target):
        return pltpu.make_async_remote_copy(
            src_ref=src,
            dst_ref=dst,
            send_sem=send_sem,
            recv_sem=recv_sem,
            device_id=target,
            device_id_type=MESH,
        )

    def row_of(c, i, side):
        return c * DEPTH + i if side == 0 else rows - 1 - c * DEPTH - i

    def staged(c, f, side):
        return (lax.rem(c, 2) * 3 + f) * lines + side * DEPTH

    def load(f, c, side):
        src = (heat_hbm, ratio_hbm, force_hbm)[f]
        first = c * DEPTH if side == 0 else rows - (c + 1) * DEPTH
        return pltpu.make_async_copy(
            src.at[pl.ds(first, DEPTH)],
            final.at[pl.ds(staged(c, f, side), DEPTH)],
            load_sem.at[f, side, lax.rem(c, 2)],
        )

    def place(z):
        return z // 2 + (z % 2) * pairs

    def planes(f, first, count):
        return (u.at[0, pl.ds(1 + first, count)], ratio.at[pl.ds(first, count)], force.at[pl.ds(first, count)])[f]

    def plane(f, n):
        return (u.at[0, 1 + n], ratio.at[n], force.at[n])[f]

    def swap_copy(f, c, at=None):
        slot = lax.rem(c, SLOTS)
        at = pl.ds(0, slab) if at is None else at
        return remote(
            packed.at[slot, f, :, at],
            planes(f, kind * pairs, pairs).at[:, c, at],
            swap_send.at[slot, f],
            swap_recv.at[c, f],
            {"lev": partner_lev},
        )

    def back_copy(c):
        return remote(
            ratio.at[pl.ds((1 - kind) * pairs, pairs), c],
            score.at[pl.ds(c * pairs, pairs)],
            back_send.at[c],
            back_recv.at[c],
            {"lev": partner_lev},
        )

    def lev_copy(p, d, c):
        src, dst = ((1, height + 1), (height, 0))[d]
        return remote(
            u.at[p, src, c],
            u.at[p, dst, c],
            lev_send.at[p, d, c],
            lev_recv.at[p, d, c],
            lev_target(d),
        )

    def lat_copy(p, d):
        return remote(
            u.at[p, pl.ds(1, height), 0, pl.ds(d * wide, wide)],
            lat_in.at[p, 1 - d],
            lat_send.at[p, d],
            lat_recv.at[p, d],
            lat_target(d),
        )

    def lon_copy(p, d, c):
        return remote(
            lon_out.at[p, d, c],
            lon_in.at[p, d, c],
            lon_send.at[p, d, c],
            lon_recv.at[p, d, c],
            lon_target(d),
        )

    def stat_copy(j, c):
        return remote(
            stat_out.at[c],
            stat_in.at[j, c],
            stat_send.at[j, c],
            stat_recv.at[j, c],
            stat_target(j),
        )

    def at_edge(c, body):
        @pl.when(c == 0)
        def _():
            for d in (0, 1):
                body(d)

    def send_faces(p, c):
        at_edge(c, lambda d: lat_copy(p, d).start())
        for d in (0, 1):
            lev_copy(p, d, c).start()
        for d in (0, 1):
            lon_copy(p, d, c).start()

    def wait_sent(p, c):
        at_edge(c, lambda d: lat_copy(p, d).wait_send())
        for d in (0, 1):
            lev_copy(p, d, c).wait_send()
            lon_copy(p, d, c).wait_send()

    def wait_faces(p, c):
        at_edge(c, lambda d: lat_copy(p, d).wait_recv())
        for d in (0, 1):
            lev_copy(p, d, c).wait_recv()
            lon_copy(p, d, c).wait_recv()

    def of_line(q):
        return pl.ds(q * wide, wide)

    def cells(z):
        return pl.ds(z, wide, stride=height)

    def put(p, c, q, z, values):
        u[p, place(z) + 1, c, of_line(q)] = values
        lon_out[p, 0, c, q * height + z] = values[0]
        lon_out[p, 1, c, q * height + z] = values[wide - 1]

    def stepped(p, c, q, z):
        i, side = q // 2, q % 2
        own = place(z) + 1
        middle = u[p, own, c, of_line(q)]
        if i == 0:
            before = u[p, own, jnp.maximum(c - 1, 0), of_line(lines - 2 + side)]
            outside = jnp.where(c == 0, lat_held[side, place(z)], before)
        else:
            outside = u[p, own, c, of_line(q - 2)]
        if i == DEPTH - 1:
            end = c == chunks - 1
            at = jnp.where(end, (lines - 1 - side) * wide, side * wide)
            inside = u[
                p, own, jnp.minimum(c + 1, chunks - 1), pl.ds(pl.multiple_of(at, wide), wide)
            ]
        else:
            inside = u[p, own, c, of_line(q + 2)]
        bottom, top = u[p, 1, c, of_line(q)], u[p, height, c, of_line(q)]
        if z == 0:
            low = swapped(jnp.where(low_lanes, top, u[p, 0, c, of_line(q)]))
        else:
            low = u[p, place(z - 1) + 1, c, of_line(q)]
        if z == height - 1:
            high = swapped(jnp.where(low_lanes, u[p, height + 1, c, of_line(q)], bottom))
        else:
            high = u[p, place(z + 1) + 1, c, of_line(q)]
        at = pl.ds(q * height + z, 1)
        west = jnp.where(first_cell, lon_in[p, 1, c, at], pltpu.roll(middle, 1, 0))
        east = jnp.where(last_cell, lon_in[p, 0, c, at], pltpu.roll(middle, wide - 1, 0))
        spread = (outside + inside) + (west + east) + (low + high) - 6.0 * middle
        return middle + ratio[own - 1, c, of_line(q)] * spread + force[own - 1, c, of_line(q)]

    def start_loads(c):
        for f in range(3):
            for side in (0, 1):
                load(f, c, side).start()

    barrier = pltpu.get_barrier_semaphore()
    second = lev - kind + 1
    near = [{**lat_target(d), "lev": second} for d in (0, 1)]
    near += [{"lev": lax.rem(second + move, lev_size)} for move in (2, lev_size - 2)]
    near += [{**stat_target(j), "lev": second} for j in range(lon_size - 1)]
    partner = {"lev": partner_lev}

    def signal(sem, other):
        pl.semaphore_signal(sem, inc=1, device_id=other, device_id_type=MESH)

    def meet_partner():
        @pl.when(kind == 0)
        def _():
            pl.semaphore_wait(barrier, 1)
            signal(met, partner)

        @pl.when(kind == 1)
        def _():
            pl.semaphore_wait(met, 1)

    def meet_all():
        @pl.when(kind == 1)
        def _():
            pl.semaphore_wait(barrier, 1 + 2 * len(near))
            signal(met, partner)

        @pl.when(kind == 0)
        def _():
            pl.semaphore_wait(met, 1)

    def pack(f, q, c):
        slot = lax.rem(c, SLOTS)
        i, side = q // 2, q % 2
        row = staged(c, f, side) + (i if side == 0 else DEPTH - 1 - i)
        for n in range(pairs):
            a, b = butterfly(final[row, cells(2 * n)], final[row, cells(2 * n + 1)])
            plane(f, kind * pairs + n)[c, of_line(q)] = jnp.where(half == 0, a, b)
            packed[slot, f, n, of_line(q)] = jnp.where(half == 0, b, a)

    def pack_all(c, meet=False):
        for f in range(3):
            for side in (0, 1):
                load(f, c, side).wait()
                for i in range(DEPTH):
                    q = 2 * i + side
                    pack(f, q, c)
                    if meet and f == 0:
                        if q == 0:
                            meet_partner()
                        swap_copy(f, c, of_line(q)).start()
            if not (meet and f == 0):
                swap_copy(f, c).start()

    start_loads(0)
    for other in [partner, *near]:
        signal(barrier, other)
    start_loads(1)
    pack_all(0, meet=True)
    start_loads(2)
    pack_all(1)
    start_loads(3)
    meet_all()

    def arrange(c):
        for f in range(3):
            swap_copy(f, c).wait_recv()
            for q in range(lines):
                for n in range(pairs):
                    at = of_line(q)
                    a, b = butterfly(plane(f, n)[c, at], plane(f, pairs + n)[c, at])
                    if f == 0:
                        put(0, c, q, 2 * n, a)
                        put(0, c, q, 2 * n + 1, b)
                    else:
                        plane(f, n)[c, at] = a
                        plane(f, pairs + n)[c, at] = b
            if f == 0:
                send_faces(0, c)

    def advance(s, c):
        p, q_ = (s - 1) % 2, s % 2
        if s >= 2:
            wait_sent(q_, c)
        wait_faces(p, c)

        @pl.when(c == 0)
        def _():
            lat_held[...] = lat_in[p]

        for q in range(lines):
            if s < STEPS:
                for z in range(height):
                    put(q_, c, q, z, stepped(p, c, q, z))
            else:
                for n in range(pairs):
                    a, b = butterfly(stepped(p, c, q, 2 * n), stepped(p, c, q, 2 * n + 1))
                    ratio[n, c, of_line(q)] = a
                    ratio[pairs + n, c, of_line(q)] = b
        if s < STEPS:
            send_faces(q_, c)
        else:
            back_copy(c).start()

    def wave(k, carry):
        @pl.when(k < chunks)
        def _():
            arrange(k)

        @pl.when(k + SLOTS < chunks)
        def _():
            c = k + SLOTS
            for f in range(3):
                swap_copy(f, c - SLOTS).wait_send()
            pack_all(c)

            @pl.when(c + 2 < chunks)
            def _():
                start_loads(c + 2)

        for s in range(1, STEPS + 1):

            @pl.when((k >= s) & (k < chunks + s))
            def _(s=s):
                advance(s, k - s)

        return carry

    lax.fori_loop(0, chunks + STEPS, wave, 0)

    def note(c, at, values):
        mean = jnp.sum(values, axis=0, keepdims=True) / wide
        apart = values - mean
        stat_out[c, pl.ds(at, 1)] = mean
        stat_out[c, pl.ds(at + height, 1)] = jnp.sum(apart * apart, axis=0, keepdims=True)

    def moments(c, q):
        at = pl.ds(2 * height * q, 2 * height)
        own = stat_out[c, at]
        others = [stat_in[j, c, at] for j in range(lon_size - 1)]
        summed = own
        for other in others:
            summed = summed + other
        mean = summed[:height] / lon_size
        apart = (own[:height] - mean) * (own[:height] - mean)
        for other in others:
            apart = apart + (other[:height] - mean) * (other[:height] - mean)
        variance = summed[height:] / (lon_size * wide) + apart / lon_size
        return mean, lax.rsqrt(variance + 0.0001)

    end = chunks - 1
    for q in range(lines):
        for z in range(height):
            note(end, 2 * height * q + z, ratio[z, end, of_line(q)])
    for j in range(lon_size - 1):
        stat_copy(j, end).start()

    def whole(c, q, n):
        own = ratio[kind * pairs + n, c, of_line(q)]
        other = score[c * pairs + n, of_line(q)]
        return butterfly(jnp.where(half == 0, own, other), jnp.where(half == 0, other, own))

    def restore(c):
        back_copy(c).wait_recv()
        for q in range(lines):
            row = row_of(c, q // 2, q % 2)
            for n in range(pairs):
                for z, values in zip((2 * n, 2 * n + 1), whole(c, q, n)):
                    final[row, cells(z)] = values
                    note(c, 2 * height * q + z, values)
        for j in range(lon_size - 1):
            stat_copy(j, c).start()

    def finish(c):
        for j in range(lon_size - 1):
            stat_copy(j, c).wait_recv()
        for q in range(lines):
            row = row_of(c, q // 2, q % 2)
            mean, scale = moments(c, q)
            for z in range(height):
                values = final[row, cells(z)]
                score[row, cells(z)] = (values - mean[z : z + 1]) * scale[z : z + 1]

    def share_moments():
        for j in range(lon_size - 1):
            stat_copy(j, end).wait_recv()
        for q in range(lines):
            mean, scale = moments(end, q)
            moment_out[q, pl.ds(0, height)] = mean
            moment_out[q, pl.ds(height, height)] = scale
        moment_copy.start()

    def last(c, carry):
        restore(c)
        pl.when(c > 0)(lambda: finish(c - 1))
        pl.when(c == 0)(share_moments)
        return carry

    moment_copy = remote(
        moment_out, moment_in, moment_send, moment_recv, {"lev": partner_lev}
    )
    lax.fori_loop(0, end, last, 0)
    finish(end - 1)

    moment_copy.wait_recv()

    def spread_out(own, other):
        a, b = jnp.where(half == 0, own, other), jnp.where(half == 0, other, own)
        first = lax.broadcasted_iota(jnp.int32, a.shape, 1) < members // 2
        return (
            jnp.where(first, a, pltpu.roll(b, members // 2, 1)),
            jnp.where(first, pltpu.roll(a, members // 2, 1), b),
        )

    back_copy(end).wait_recv()
    for n in range(pairs):
        for q in range(lines):
            row = row_of(end, q // 2, q % 2)
            for z, values in zip((2 * n, 2 * n + 1), whole(end, q, n)):
                final[row, cells(z)] = values
    for n in range(pairs):
        for q in range(lines):
            row = row_of(end, q // 2, q % 2)
            ours = kind * pairs + n
            means, scales = (
                spread_out(moment_out[q, pl.ds(o + ours, 1)], moment_in[q, pl.ds(o + ours, 1)])
                for o in (0, height)
            )
            for z, m, k in zip((2 * n, 2 * n + 1), means, scales):
                score[row, cells(z)] = (final[row, cells(z)] - m) * k

    def settle(c, carry):
        wait_sent((STEPS - 1) % 2, c)
        back_copy(c).wait_send()
        for j in range(lon_size - 1):
            stat_copy(j, c).wait_send()
        return carry

    lax.fori_loop(0, chunks, settle, 0)
    moment_copy.wait_send()
    for c in range(chunks - SLOTS, chunks):
        for f in range(3):
            swap_copy(f, c).wait_send()


def write_out(score, final, score_hbm, final_hbm, sem):
    rows = score.shape[0] // PARTS
    copies = [
        pltpu.make_async_copy(
            src.at[pl.ds(i * rows, rows)], dst.at[pl.ds(i * rows, rows)], sem.at[n, i]
        )
        for i in range(PARTS)
        for n, (src, dst) in enumerate(((score, score_hbm), (final, final_hbm)))
    ]
    for copy in copies:
        copy.start()
    for copy in copies:
        copy.wait()


def local(sizes, initial_heat, diffusivity_ratio, forcing_term):
    rows, wide, height, members = initial_heat.shape
    flat = (rows, wide * height, members)
    chunks, slab = rows // (2 * DEPTH), 2 * DEPTH * wide
    hbm = pl.BlockSpec(memory_space=pl.ANY)
    vmem = pl.BlockSpec(memory_space=pltpu.VMEM)
    f32, dma = jnp.float32, pltpu.SemaphoreType.DMA
    others, pairs = sizes[1] - 1, height // 2
    score, final = pl.pallas_call(
        functools.partial(kernel, sizes),
        out_shape=(pltpu.VMEM(flat, f32), pltpu.VMEM(flat, f32)),
        in_specs=[hbm, hbm, hbm],
        out_specs=(vmem, vmem),
        scratch_shapes=[
            pltpu.VMEM((2, height + 2, chunks, slab, members), f32),
            pltpu.VMEM((height, chunks, slab, members), f32),
            pltpu.VMEM((height, chunks, slab, members), f32),
            pltpu.VMEM((SLOTS, 3, pairs, slab, members), f32),
            pltpu.VMEM((2, 2, height, wide, members), f32),
            pltpu.VMEM((2, height, wide, members), f32),
            pltpu.VMEM((2, 2, chunks, 2 * DEPTH * height, members), f32),
            pltpu.VMEM((2, 2, chunks, 2 * DEPTH * height, members), f32),
            pltpu.VMEM((chunks, 4 * DEPTH * height, members), f32),
            pltpu.VMEM((others, chunks, 4 * DEPTH * height, members), f32),
            pltpu.VMEM((2 * DEPTH, 2 * height, members), f32),
            pltpu.VMEM((2 * DEPTH, 2 * height, members), f32),
            dma((3, 2, 2)),
            dma((SLOTS, 3)),
            dma((chunks, 3)),
            dma((chunks,)),
            dma((chunks,)),
            dma((2, 2, chunks)),
            dma((2, 2, chunks)),
            dma((2, 2, chunks)),
            dma((2, 2, chunks)),
            dma((2, 2)),
            dma((2, 2)),
            dma((others, chunks)),
            dma((others, chunks)),
            dma,
            dma,
            pltpu.SemaphoreType.REGULAR,
        ],
        compiler_params=pltpu.CompilerParams(
            collective_id=0, has_side_effects=True, vmem_limit_bytes=int(47.25 * 2**20)
        ),
    )(*(a.reshape(flat) for a in (initial_heat, diffusivity_ratio, forcing_term)))
    score, final = pl.pallas_call(
        write_out,
        out_shape=(jax.ShapeDtypeStruct(flat, f32), jax.ShapeDtypeStruct(flat, f32)),
        in_specs=[vmem, vmem],
        out_specs=(hbm, hbm),
        scratch_shapes=[dma((2, PARTS))],
        compiler_params=pltpu.CompilerParams(vmem_limit_bytes=4 * 2**20),
    )(*(pltpu.with_memory_space_constraint(a, pltpu.VMEM) for a in (score, final)))
    return score.reshape(initial_heat.shape), final.reshape(initial_heat.shape)


def solution(mesh):
    sizes = tuple(mesh.shape[a] for a in ("lat", "lon", "lev"))
    placed = P("lat", "lon", "lev", None)
    return jax.shard_map(
        functools.partial(local, sizes),
        mesh=mesh,
        in_specs=(placed, placed, placed),
        out_specs=(placed, placed),
        check_vma=False,
    )
```
